32 devices in a mesh: leaf: 8 (over z, y), probe: 4 (over x, core).
Axes of the slice: x: 2, y: 2, z: 4, core: 2. Of those that a mesh axis runs over, the one named last changes fastest.
Arguments:
- coords: float32 [3, 32768], P(None, 'leaf')
- site_order: int32 [128, 256], P('leaf'), may hold values from 0 to 255, each once within a row
- leaf_pairs: int32 [2, 768], P(None, 'leaf'), may hold values from 0 to 127, as said below
- pair_count: int32 [8], P('leaf'), may hold values from 31 to 96, as said below
- probes: float32 [64, 32768], P('probe', 'leaf'), may hold values from -16 to 16
Outputs:
- solution: float32 [64, 32768], P('probe', 'leaf')
- residual: float32 [64, 32768], P('probe', 'leaf')
The draws below stay inside these ranges and needn't reach their ends.
Inputs may be any that keep to these rules, and one draw needn't show every extreme that they name: `leaf_pairs`: each leaf index owns 96 slots; its first pair_count slots hold distinct pairs (i, j) with i among that index's own 16 leaves and i <= j <= i + 5, j < 128, every own leaf listed with itself once and with the next leaf where there is one; the later slots hold the index's first leaf twice. `pair_count`: pairs listed for each leaf index; some index lists 96 in every draw. Each row of site_order lists 0 to 255 once.
All inputs are finite; a program needn't handle non-finite values.
Results may differ from the reference program's by a relative error of at most 0.0003.
Values sent between devices are 32-bit elements; how exact they have to be, the bound alone decides.
A program may use at most 64 MiB of HBM per device.

```python
import math
import jax
import jax.numpy as jnp
from jax import lax

LEAF = 256
REACH = 5
PROBES = 64
ITERS = 2
LEAF_DEV = 16
LEAVES = 128
SITES = 32768


UNIT = 0.025


SIDE = 0.5


def slab_layout(key):
    groups = LEAVES // LEAF_DEV
    k_wide, k_dense, k_force = jax.random.split(jax.random.fold_in(key, 7), 3)
    widths = jax.random.randint(k_wide, (LEAVES,), 2, REACH + 1)
    flagged = jax.random.randint(k_dense, (groups,), 0, 8) == 0
    forced = jax.random.randint(k_force, (), 0, groups - 1)
    leaf_ids = jnp.arange(LEAVES)
    owner = leaf_ids // LEAF_DEV
    follow = (leaf_ids >= (forced + 1) * LEAF_DEV) & (leaf_ids < (forced + 1) * LEAF_DEV + REACH - 1)
    crowded = flagged[owner] | (owner == forced) | follow
    widths = jnp.where(crowded, 1, widths)
    ends = jnp.cumsum(widths)
    start_offsets = ends - widths
    return (widths, start_offsets, ends)


def pair_table(key):
    widths, start_offsets, ends = slab_layout(key)
    groups = LEAVES // LEAF_DEV
    slots = LEAF_DEV * (REACH + 1)
    leaf_ids = jnp.arange(LEAVES)
    offsets = jnp.arange(REACH + 1)
    partner = leaf_ids[:, None] + offsets[None, :]
    inside = partner < LEAVES
    capped = jnp.minimum(partner, LEAVES - 1)
    near = start_offsets[capped] - ends[:, None] < REACH
    valid = (inside & ((offsets[None, :] == 0) | near)).reshape(groups, slots)
    rows = jnp.broadcast_to(leaf_ids[:, None], partner.shape).reshape(groups, slots)
    cols = capped.reshape(groups, slots)
    sorted_rank = jnp.argsort(1 - valid.astype(jnp.int32), axis=1, stable=True)
    rows = jnp.take_along_axis(rows, sorted_rank, axis=1)
    cols = jnp.take_along_axis(cols, sorted_rank, axis=1)
    count = jnp.sum(valid.astype(jnp.int32), axis=1)
    live = jnp.arange(slots)[None, :] < count[:, None]
    first = (jnp.arange(groups) * LEAF_DEV)[:, None]
    rows = jnp.where(live, rows, first)
    cols = jnp.where(live, cols, first)
    return (jnp.stack([rows.reshape(-1), cols.reshape(-1)]).astype(jnp.int32), count.astype(jnp.int32))


def draw_leaf_pairs(key, part):
    return pair_table(key)[0]


def draw_pair_count(key, part):
    return pair_table(key)[1]


def draw_coords(key, part):
    widths, start_offsets, ends = slab_layout(key)
    k_along, k_across = jax.random.split(jax.random.fold_in(key, 11))
    along = jax.random.uniform(k_along, (LEAVES, LEAF), jnp.float32)
    first = (start_offsets[:, None].astype(jnp.float32) + widths[:, None].astype(jnp.float32) * along) * UNIT
    across = jax.random.uniform(k_across, (2, LEAVES, LEAF), jnp.float32) * SIDE
    return jnp.concatenate([first[None], across], axis=0).reshape(3, SITES).astype(jnp.float32)


def draw_probes(key, part):
    k_base, k_row, k_leaf = jax.random.split(jax.random.fold_in(key, 13), 3)
    base = jnp.clip(jax.random.normal(k_base, (PROBES, LEAVES, LEAF), jnp.float32), -4.0, 4.0)
    row_scale = jnp.exp(jax.random.uniform(k_row, (PROBES, 1, 1), jnp.float32, -1.15, 1.15))
    leaf_scale = jnp.exp(jax.random.uniform(k_leaf, (1, LEAVES, 1), jnp.float32, -1.15, 1.15))
    rising = jnp.exp(0.55 * jnp.arange(LEAVES, dtype=jnp.float32) / LEAVES)[None, :, None]
    values = jnp.clip(base * row_scale * leaf_scale * rising, -16.0, 16.0)
    return values.reshape(PROBES, SITES).astype(jnp.float32)


def setup_inputs(seed: int = 0) -> dict:
    streams_of = jax.random.split(jax.random.key(seed), 6)
    return {
        "coords": draw_coords(jax.random.fold_in(streams_of[5], 71), 0),
        "site_order": jax.vmap(lambda own: jax.random.permutation(own, LEAF))(jax.random.split(streams_of[1], LEAVES)).reshape((LEAVES, LEAF)).astype(jnp.int32),
        "leaf_pairs": draw_leaf_pairs(jax.random.fold_in(streams_of[5], 71), 0),
        "pair_count": draw_pair_count(jax.random.fold_in(streams_of[5], 71), 0),
        "probes": draw_probes(jax.random.fold_in(streams_of[5], 71), 0),
    }


UNIT = 0.025
LENGTH = 0.12
NUGGET = 0.5
UPPER_LIMIT = lax.Precision.HIGHEST

def kernel_tiles(left, right):
    diff = left[:, :, :, None] - right[:, :, None, :]
    dist = jnp.sqrt(lax.optimization_barrier(jnp.sum(diff * diff, axis=0)))
    taper = REACH * UNIT
    scaled = dist * (math.sqrt(3.0) / LENGTH)
    remain = jnp.maximum(1.0 - dist / taper, 0.0)
    return (1.0 + scaled) * jnp.exp(-scaled) * remain ** 4 * (1.0 + 4.0 * dist / taper)

def apply_operator(points, leaf_pairs, pair_count, field):
    groups = pair_count.shape[0]
    slots = leaf_pairs.shape[1] // groups

    def one_group(group, grand_total):

        def one_pair(index, acc):
            slot = group * slots + index
            row = leaf_pairs[0, slot]
            col = leaf_pairs[1, slot]
            tile = kernel_tiles(points[:, row][:, None], points[:, col][:, None])[0]
            to_row = jnp.dot(field[:, col], tile.T, precision=UPPER_LIMIT)
            column_target = jnp.dot(field[:, row], tile, precision=UPPER_LIMIT)
            column_target = jnp.where(row != col, column_target, jnp.zeros_like(column_target))
            acc = acc.at[:, row].add(to_row)
            return acc.at[:, col].add(column_target)
        return lax.fori_loop(0, pair_count[group], one_pair, grand_total)
    summed = lax.fori_loop(0, groups, one_group, jnp.zeros_like(field))
    return NUGGET * field + summed

def reference(coords, site_order, leaf_pairs, pair_count, probes):
    points = jnp.take_along_axis(coords.reshape(3, LEAVES, LEAF), site_order[None], axis=2)
    right = probes.reshape(PROBES, LEAVES, LEAF)
    solution = jnp.zeros_like(right)
    residual = right
    direction = right
    norm_now = lax.optimization_barrier(jnp.sum(residual * residual, axis=(1, 2)))
    for step in range(ITERS):
        image = apply_operator(points, leaf_pairs, pair_count, direction)
        alpha = norm_now / lax.optimization_barrier(jnp.sum(direction * image, axis=(1, 2)))
        solution = solution + alpha[:, None, None] * direction
        residual = residual - alpha[:, None, None] * image
        if step + 1 < ITERS:
            norm_next = lax.optimization_barrier(jnp.sum(residual * residual, axis=(1, 2)))
            direction = residual + (norm_next / norm_now)[:, None, None] * direction
            norm_now = norm_next
    return (solution.reshape(PROBES, SITES), residual.reshape(PROBES, SITES))
```

```python
import functools
import math

import jax
import jax.numpy as jnp
from jax import lax
from jax.experimental import pallas as pl
from jax.experimental.pallas import tpu as pltpu
from jax.sharding import PartitionSpec as P

REACH = 5
UNIT = 0.025
LENGTH = 0.12
NUGGET = 0.5
SHIFT = NUGGET + 1.0
TAPER = REACH * UNIT
GROW = math.sqrt(3.0) * TAPER / LENGTH
RATE = GROW / math.log(2.0)
QUAD = 4.0 * GROW
LIN = -(4.0 + 9.0 * GROW) * RATE / QUAD
CON = 5.0 * (1.0 + GROW) * RATE**2 / QUAD
NORM = QUAD * 2.0**-RATE / RATE**6
OFFS = REACH + 1
ROWS = 32
MESH = pl.DeviceIdType.MESH
F32 = jnp.float32
BF16 = jnp.bfloat16


def dot(a, b, ca, cb):
    return lax.dot_general(a, b, (((ca,), (cb,)), ((), ())), preferred_element_type=F32)


def three(x, axis):
    hi = x.astype(BF16).astype(F32)
    mid = (x - hi).astype(BF16).astype(F32)
    return jnp.concatenate([hi, mid, x - hi - mid], axis=axis).astype(BF16)


def kernel(
    n, coords_hbm, order_hbm, pairs_hbm, count_hbm, probes_hbm, sol_ref, res_ref,
    cin, order, pairs, count, own, c8, prow, pcb, mask, tiles, d, w, wfar, v2, acc, acc2,
    in_low, in_high, part, back, sum_out, sum_in, isem, ssem, rsem, hsend, hrecv,
):
    leaf_dev, width = order.shape
    cols = probes_hbm.shape[0]
    half = leaf_dev // 2
    span = half + REACH
    me = lax.axis_index("leaf")
    probe = lax.axis_index("probe")
    mine = lax.rem(probe, 2)
    other = 1 - mine
    even = probe - mine
    twin = even + other
    base = half * mine
    twin_base = half * other
    after = lax.rem(me + 1, n)
    before = lax.rem(me + n - 1, n)
    low_leaf = jnp.where(mine == 0, before, me)
    high_leaf = jnp.where(mine == 0, me, after)
    has_low = jnp.logical_or(mine == 1, me > 0)
    has_high = jnp.logical_or(mine == 0, me < n - 1)

    peers = [(k - 1, lax.rem(me + k, n), probe) for k in range(1, n)]
    peers += [(n - 1 + k, lax.rem(me + k, n), twin) for k in range(n)]
    slots_in = len(peers)

    def load(src, dst, slot):
        return pltpu.make_async_copy(src, dst, isem.at[slot])

    loads = [
        load(coords_hbm, cin, 0), load(order_hbm, order, 1), load(pairs_hbm, pairs, 2),
        load(count_hbm, count, 3),
    ]
    for l in range(leaf_dev):
        loads.append(load(probes_hbm.at[:, l * width : (l + 1) * width], own.at[l], 4 + l))
    for copy in loads:
        copy.start()
    barrier = pltpu.get_barrier_semaphore()
    for _, leaf, row in peers:
        pl.semaphore_signal(
            barrier, inc=1, device_id={"leaf": leaf, "probe": row}, device_id_type=MESH
        )

    def hop(src, dst, slot, leaf, row, landing=None):
        return pltpu.make_async_remote_copy(
            src_ref=src, dst_ref=dst, send_sem=hsend.at[slot],
            recv_sem=hrecv.at[slot if landing is None else landing],
            device_id={"leaf": leaf, "probe": row}, device_id_type=MESH,
        )

    place = lax.broadcasted_iota(jnp.int32, (width, width), 0)
    for copy in loads[:4]:
        copy.wait()
    c8[...] = jnp.zeros_like(c8)
    c8[0:3, :] = cin[...] * (RATE / TAPER)

    def gather(k):
        x = c8[:, pl.ds(pl.multiple_of((base + k) * width, width), width)]
        parts = three(x, 0)
        onehot = jnp.where(place == order[pl.ds(base + k, 1), :], 1.0, 0.0).astype(BF16)
        got = dot(parts, onehot, 1, 0)
        prow[k] = got[0:8] + got[8:16] + got[16:24]

    for k in range(half):
        gather(k)

    @pl.when(mine == 0)
    def _():
        for k in range(half, span):
            gather(k)

    slots = pairs.shape[1]
    first = pairs[0:1, :]
    second = pairs[1:2, :]
    code = (first - me * leaf_dev - base) * OFFS + (second - first)
    lane = lax.broadcasted_iota(jnp.int32, (1, slots), 1)
    code = jnp.where(lane < count[0], code, -1)
    want = lax.broadcasted_iota(jnp.int32, (half * OFFS, slots), 0)
    hit = jnp.max(jnp.where(want == code, RATE, 0.0), axis=1, keepdims=True)
    mask[...] = jnp.broadcast_to(hit, mask.shape)
    acc[...] = jnp.zeros_like(acc)
    acc2[...] = jnp.zeros_like(acc2)

    def both(field, k):
        return jnp.concatenate([field[0, k], field[1, k]], axis=0)

    def stack(k, x):
        hi = x.astype(BF16)
        v2[k] = jnp.concatenate([hi, (x - hi.astype(F32)).astype(BF16)], axis=0)

    def add(into, k, x):
        into[0, k] += x[:cols]
        into[1, k] += x[cols:]

    rows = 2 * cols

    def products(i, into):
        vi = v2[i]
        row = jnp.zeros((2 * rows, width), F32)
        low = jnp.zeros((rows, width), F32)
        for o in range(OFFS):
            hi = tiles[i * OFFS + o, 0]
            lo = tiles[i * OFFS + o, 1]
            vj = v2[i + o]
            row = row + dot(vj, hi, 1, 1)
            low = low + dot(vj[:rows], lo, 1, 1)
            if o > 0:
                col = dot(vi, hi, 1, 0)
                add(into, i + o, col[:rows] + col[rows:] + dot(vi[:rows], lo, 1, 0))
        add(into, i, row[:rows] + row[rows:] + low)

    def build(i):
        turned = prow[i].T
        for c in range(3):
            pcb[c] = jnp.broadcast_to(turned[:, c : c + 1], (width, 128))
        for o in range(OFFS):
            s = i * OFFS + o
            for h in range(0, width, 128):
                listed = mask[pl.ds(s, 1), :]
                right = [
                    jnp.broadcast_to(
                        jnp.where(
                            listed > 0.0,
                            prow[i + o, c : c + 1, h : h + 128],
                            prow[i, c : c + 1, h : h + 128],
                        ),
                        (ROWS, 128),
                    )
                    for c in range(3)
                ]
                top = jnp.broadcast_to(listed, (ROWS, 128))
                for a in range(0, width, ROWS):
                    dx = pcb[0, a : a + ROWS, :] - right[0]
                    dy = pcb[1, a : a + ROWS, :] - right[1]
                    dz = pcb[2, a : a + ROWS, :] - right[2]
                    d2 = jnp.maximum(dx * dx + dy * dy + dz * dz, 1e-30)
                    y = jnp.maximum(top - d2 * lax.rsqrt(d2), 0.0)
                    y2 = y * y
                    t = (y2 * y2) * (y2 + (LIN * y + CON)) * jnp.exp2(y)
                    hi = t.astype(BF16)
                    tiles[s, 0, a : a + ROWS, h : h + 128] = hi
                    tiles[s, 1, a : a + ROWS, h : h + 128] = (t - hi.astype(F32)).astype(BF16)

    build(0)

    for copy in loads[4:]:
        copy.wait()
    pl.semaphore_wait(barrier, slots_in)

    point_hop = hop(prow.at[pl.ds(0, REACH)], prow.at[pl.ds(half, REACH)], 0, before, twin)
    rim_hop = hop(own.at[pl.ds(0, REACH)], d.at[mine, pl.ds(half, REACH)], 1, before, even + 1, 1 + mine)
    rim_in = [
        hop(own.at[pl.ds(0, REACH)], d.at[k, pl.ds(half, REACH)], 1, before, even + 1, 1 + k)
        for k in range(2)
    ]
    twin_hop = hop(own.at[pl.ds(twin_base, half)], d.at[mine, pl.ds(0, half)], 3, me, twin)
    ring_hop = hop(own.at[pl.ds(half, REACH)], d.at[mine, pl.ds(half, REACH)], 4, me, twin)
    twin_hop.start()

    @pl.when(mine == 1)
    def _():
        ring_hop.start()

    @pl.when(jnp.logical_and(mine == 0, me > 0))
    def _():
        point_hop.start()

    @pl.when(me > 0)
    def _():
        rim_hop.start()

    for k in range(half):
        d[mine, k] = own[base + k]

    @pl.when(mine == 0)
    def _():
        for k in range(half, span):
            d[0, k] = own[k]

    @pl.when(jnp.logical_and(mine == 1, me == n - 1))
    def _():
        d[:, pl.ds(half, REACH)] = jnp.zeros((2, REACH, cols, width), F32)
        prow[pl.ds(half, REACH)] = jnp.zeros((REACH, 8, width), F32)

    twin_hop.wait_recv()
    for k in range(half):
        stack(k, both(d, k))

    low_hop = hop(acc.at[:, pl.ds(0, REACH)], in_high, 5, low_leaf, twin)
    high_hop = hop(acc.at[:, pl.ds(half, REACH)], in_low, 6, high_leaf, twin)

    def first_pass(i, carry):
        @pl.when(jnp.logical_and(i == half - REACH, jnp.logical_and(mine == 1, me < n - 1)))
        def _():
            point_hop.wait_recv()

        @pl.when(i == half - REACH + 1)
        def _():
            @pl.when(mine == 0)
            def _():
                ring_hop.wait_recv()

            @pl.when(jnp.logical_and(mine == 1, me < n - 1))
            def _():
                for k in range(2):
                    rim_in[k].wait_recv()

            for k in range(half, span):
                stack(k, both(d, k))

        build(i)
        products(i - 1, acc)

        @pl.when(jnp.logical_and(i == REACH, has_low))
        def _():
            low_hop.start()

        return carry

    lax.fori_loop(1, half, first_pass, 0)
    products(half - 1, acc)

    @pl.when(has_high)
    def _():
        high_hop.start()

    @pl.when(jnp.logical_not(has_low))
    def _():
        in_low[...] = jnp.zeros_like(in_low)

    @pl.when(jnp.logical_not(has_high))
    def _():
        in_high[...] = jnp.zeros_like(in_high)

    def make_w(k, more):
        xs = []
        for r in range(2):
            x = acc[r, k]
            if more is not None:
                x = x + more[r]
            x = NORM * x - d[r, k]
            w[r, k] = x
            xs.append(x)
        stack(k, jnp.concatenate(xs, axis=0))

    for k in range(REACH, half):
        make_w(k, None)

    @pl.when(has_high)
    def _():
        low_hop.wait_recv()

    for k in range(half, span):
        make_w(k, [in_high[r, k - half] for r in range(2)])

    @pl.when(has_low)
    def _():
        high_hop.wait_recv()

    for k in range(REACH):
        make_w(k, [in_low[r, k] for r in range(2)])

    far_hop = hop(w.at[other, pl.ds(0, half)], wfar, 7, me, twin)
    far_hop.start()

    def second_pass(i, carry):
        products(i, acc2)
        return carry

    lax.fori_loop(0, half, second_pass, 0)

    give_hop = hop(acc2.at[other, pl.ds(0, half)], part.at[pl.ds(0, half)], 8, me, twin)
    give_rim = hop(acc2.at[other, pl.ds(half, REACH)], part.at[pl.ds(half, REACH)], 9, me, twin)
    next_even = hop(acc2.at[0, pl.ds(half, REACH)], part.at[pl.ds(half, REACH)], 9, after, even)
    next_odd = hop(acc2.at[1, pl.ds(half, REACH)], back, 10, after, even + 1)
    give_hop.start()

    @pl.when(mine == 0)
    def _():
        give_rim.start()

    @pl.when(jnp.logical_and(mine == 1, me < n - 1))
    def _():
        next_even.start()
        next_odd.start()

    def lanes(x):
        return x[:, :128] + x[:, 128:] if width == 256 else x

    sums = [jnp.zeros((rows, width), F32) for _ in range(4)]
    for k in range(span):
        wk = both(w, k)
        sums[3] = sums[3] + wk * both(acc2, k)
        if k < half:
            dk = both(d, k)
            sums[0] = sums[0] + dk * dk
            sums[1] = sums[1] + dk * wk
            sums[2] = sums[2] + wk * wk
    stacked = jnp.concatenate([lanes(x) for x in sums], axis=0)
    parts = three(stacked, 1)
    total = dot(jnp.full((8, parts.shape[1]), 1.0, BF16), parts, 1, 1)
    sum_out[...] = total[0:1]
    copies = []
    for slot, leaf, row in peers:
        copy = pltpu.make_async_remote_copy(
            src_ref=sum_out, dst_ref=sum_in.at[slot],
            send_sem=ssem.at[slot], recv_sem=rsem.at[slot],
            device_id={"leaf": leaf, "probe": row}, device_id_type=MESH,
        )
        copy.start()
        copies.append(copy)

    @pl.when(jnp.logical_and(mine == 0, me == 0))
    def _():
        part[pl.ds(half, REACH)] = jnp.zeros((REACH, cols, width), F32)

    @pl.when(jnp.logical_and(mine == 1, me == 0))
    def _():
        back[...] = jnp.zeros_like(back)

    @pl.when(mine == 0)
    def _():
        back[...] = acc2[0, pl.ds(half, REACH)]

    total = sum_out[...]
    for slot, copy in enumerate(copies):
        copy.wait_recv()
        total = total + sum_in[slot]
    seat = lax.broadcasted_iota(jnp.int32, (cols, 128), 1)
    line = lax.broadcasted_iota(jnp.int32, (cols, 128), 0) + mine * cols
    rr, dw, ww, wk = [
        jnp.sum(jnp.where(seat == line + q * rows, total, 0.0), axis=1, keepdims=True)
        for q in range(4)
    ]
    wz = NORM * wk - ww
    m = dw / rr
    alpha0 = rr / (SHIFT * rr + dw)
    uu = ww - m * dw
    tilt = alpha0 * uu / rr
    alpha1 = uu / (SHIFT * uu + (m * (m * dw - 2.0 * ww) + wz) - tilt * uu)
    e = alpha0 * (m + tilt)
    both_alpha = alpha0 * alpha1
    sol_d = alpha0 + alpha1 * e
    res_d = alpha0 * m - SHIFT * alpha1 * e
    res_w = -(alpha0 + alpha1 * e - SHIFT * both_alpha) - both_alpha
    res_z = both_alpha * NORM

    far_hop.wait_recv()
    give_hop.wait_recv()

    @pl.when(mine == 1)
    def _():
        give_rim.wait_recv()

    @pl.when(jnp.logical_and(mine == 0, me > 0))
    def _():
        next_even.wait_recv()

    @pl.when(jnp.logical_and(mine == 1, me > 0))
    def _():
        next_odd.wait_recv()

    def finish(l, dl, wl, zl):
        at = pl.ds(pl.multiple_of(l * width, width), width)
        sol_ref[:, at] = sol_d * dl - both_alpha * wl
        res_ref[:, at] = res_d * dl + res_w * wl + res_z * zl

    for k in range(half):
        near = acc2[mine, k]
        far = part[k]
        if k < REACH:
            near = near + part[half + k]
            far = far + back[k]
        finish(base + k, d[mine, k], w[mine, k], near)
        finish(twin_base + k, own[twin_base + k], wfar[k], far)

    for copy in copies:
        copy.wait_send()
    for copy in (twin_hop, far_hop, give_hop):
        copy.wait_send()

    @pl.when(mine == 1)
    def _():
        ring_hop.wait_send()

    @pl.when(mine == 0)
    def _():
        give_rim.wait_send()

    @pl.when(jnp.logical_and(mine == 0, me > 0))
    def _():
        point_hop.wait_send()

    @pl.when(me > 0)
    def _():
        rim_hop.wait_send()

    @pl.when(has_low)
    def _():
        low_hop.wait_send()

    @pl.when(has_high)
    def _():
        high_hop.wait_send()

    @pl.when(jnp.logical_and(mine == 1, me < n - 1))
    def _():
        next_even.wait_send()
        next_odd.wait_send()


def body(coords, site_order, leaf_pairs, pair_count, probes):
    n = lax.axis_size("leaf")
    leaf_dev, width = site_order.shape
    cols = probes.shape[0]
    half = leaf_dev // 2
    span = half + REACH
    slots_in = 2 * n - 1
    hbm = pl.BlockSpec(memory_space=pl.ANY)
    vmem = pl.BlockSpec(memory_space=pltpu.VMEM)
    field = functools.partial(pltpu.VMEM, dtype=F32)
    return pl.pallas_call(
        functools.partial(kernel, n),
        out_shape=(jax.ShapeDtypeStruct(probes.shape, F32),) * 2,
        in_specs=[hbm] * 5,
        out_specs=(vmem, vmem),
        scratch_shapes=[
            field(coords.shape),
            pltpu.VMEM(site_order.shape, jnp.int32),
            pltpu.VMEM(leaf_pairs.shape, jnp.int32),
            pltpu.SMEM(pair_count.shape, jnp.int32),
            field((leaf_dev, cols, width)),
            field((8, leaf_dev * width)),
            field((span, 8, width)),
            field((3, width, 128)),
            field((half * OFFS, 128)),
            pltpu.VMEM((half * OFFS, 2, width, width), BF16),
            field((2, span, cols, width)),
            field((2, span, cols, width)),
            field((half, cols, width)),
            pltpu.VMEM((span, 4 * cols, width), BF16),
            field((2, span, cols, width)),
            field((2, span, cols, width)),
            field((2, REACH, cols, width)),
            field((2, REACH, cols, width)),
            field((span, cols, width)),
            field((REACH, cols, width)),
            field((1, 128)),
            field((slots_in, 1, 128)),
            pltpu.SemaphoreType.DMA((4 + leaf_dev,)),
            pltpu.SemaphoreType.DMA((slots_in,)),
            pltpu.SemaphoreType.DMA((slots_in,)),
            pltpu.SemaphoreType.DMA((11,)),
            pltpu.SemaphoreType.DMA((11,)),
        ],
        compiler_params=pltpu.CompilerParams(
            collective_id=0, has_side_effects=True, vmem_limit_bytes=48 * 2**20
        ),
    )(coords, site_order, leaf_pairs, pair_count, probes)


def solution(mesh):
    in_specs = (P(None, "leaf"), P("leaf", None), P(None, "leaf"), P("leaf"), P("probe", "leaf"))
    out_specs = (P("probe", "leaf"), P("probe", "leaf"))
    return jax.shard_map(body, mesh=mesh, in_specs=in_specs, out_specs=out_specs, check_vma=False)
```

```python
import functools
import math

import jax
import jax.numpy as jnp
from jax import lax
from jax.experimental import pallas as pl
from jax.experimental.pallas import tpu as pltpu
from jax.sharding import PartitionSpec as P

REACH = 5
UNIT = 0.025
LENGTH = 0.12
NUGGET = 0.5
SHIFT = NUGGET + 1.0
TAPER = REACH * UNIT
GROW = math.sqrt(3.0) * TAPER / LENGTH
RATE = GROW / math.log(2.0)
QUAD = 4.0 * GROW
LIN = -(4.0 + 9.0 * GROW) * RATE / QUAD
CON = 5.0 * (1.0 + GROW) * RATE**2 / QUAD
NORM = QUAD * 2.0**-RATE / RATE**6
OFFS = REACH + 1
ROWS = 32
MESH = pl.DeviceIdType.MESH
F32 = jnp.float32
BF16 = jnp.bfloat16


def dot(a, b, ca, cb):
    return lax.dot_general(a, b, (((ca,), (cb,)), ((), ())), preferred_element_type=F32)


def three(x, axis):
    hi = x.astype(BF16).astype(F32)
    mid = (x - hi).astype(BF16).astype(F32)
    return jnp.concatenate([hi, mid, x - hi - mid], axis=axis).astype(BF16)


def kernel(
    n, coords_hbm, order_hbm, pairs_hbm, probes_hbm, sol_ref, res_ref,
    cin, order, pairs, own, c8, prow, pcb, mask, tiles, d, w, wfar, v2, acc, acc2,
    in_low, in_high, part, back, diag, sum_out, sum_in, isem, ssem, rsem, hsend, hrecv,
):
    leaf_dev, width = order.shape
    cols = probes_hbm.shape[0]
    half = leaf_dev // 2
    span = half + REACH
    me = lax.axis_index("leaf")
    probe = lax.axis_index("probe")
    mine = lax.rem(probe, 2)
    other = 1 - mine
    even = probe - mine
    twin = even + other
    base = half * mine
    twin_base = half * other
    after = lax.rem(me + 1, n)
    before = lax.rem(me + n - 1, n)
    low_leaf = jnp.where(mine == 0, before, me)
    high_leaf = jnp.where(mine == 0, me, after)
    has_low = jnp.logical_or(mine == 1, me > 0)
    has_high = jnp.logical_or(mine == 0, me < n - 1)

    peers = [(k - 1, lax.rem(me + k, n), probe) for k in range(1, n)]
    peers += [(n - 1 + k, lax.rem(me + k, n), twin) for k in range(n)]
    slots_in = len(peers)

    def load(src, dst, slot):
        return pltpu.make_async_copy(src, dst, isem.at[slot])

    loads = [
        load(coords_hbm, cin, 0), load(order_hbm, order, 1), load(pairs_hbm, pairs, 2),
    ]
    for l in range(leaf_dev):
        loads.append(load(probes_hbm.at[:, l * width : (l + 1) * width], own.at[l], 3 + l))
    for copy in loads:
        copy.start()
    barrier = pltpu.get_barrier_semaphore()
    for _, leaf, row in peers:
        pl.semaphore_signal(
            barrier, inc=1, device_id={"leaf": leaf, "probe": row}, device_id_type=MESH
        )

    def hop(src, dst, slot, leaf, row, landing=None):
        return pltpu.make_async_remote_copy(
            src_ref=src, dst_ref=dst, send_sem=hsend.at[slot],
            recv_sem=hrecv.at[slot if landing is None else landing],
            device_id={"leaf": leaf, "probe": row}, device_id_type=MESH,
        )

    for copy in loads[3:]:
        copy.wait()
    pl.semaphore_wait(barrier, slots_in)

    point_hop = hop(prow.at[pl.ds(0, REACH)], prow.at[pl.ds(half, REACH)], 0, before, twin)
    rim_hop = hop(own.at[pl.ds(0, REACH)], d.at[mine, pl.ds(half, REACH)], 1, before, even + 1, 1 + mine)
    rim_in = [
        hop(own.at[pl.ds(0, REACH)], d.at[k, pl.ds(half, REACH)], 1, before, even + 1, 1 + k)
        for k in range(2)
    ]
    twin_hop = hop(own.at[pl.ds(twin_base, half)], d.at[mine, pl.ds(0, half)], 3, me, twin)
    ring_hop = hop(own.at[pl.ds(half, REACH)], d.at[mine, pl.ds(half, REACH)], 4, me, twin)
    twin_hop.start()

    @pl.when(mine == 1)
    def _():
        ring_hop.start()

    @pl.when(me > 0)
    def _():
        rim_hop.start()

    place = lax.broadcasted_iota(jnp.int32, (width, width), 0)
    for copy in loads[:3]:
        copy.wait()
    c8[...] = jnp.zeros_like(c8)
    c8[0:3, :] = cin[...] * (RATE / TAPER)

    def gather(k):
        x = c8[:, pl.ds(pl.multiple_of((base + k) * width, width), width)]
        parts = three(x, 0)
        onehot = jnp.where(place == order[pl.ds(base + k, 1), :], 1.0, 0.0).astype(BF16)
        got = dot(parts, onehot, 1, 0)
        prow[k] = got[0:8] + got[8:16] + got[16:24]

    for k in range(half):
        gather(k)

    @pl.when(mine == 0)
    def _():
        for k in range(half, span):
            gather(k)

    slots = pairs.shape[1]
    first = pairs[0:1, :]
    second = pairs[1:2, :]
    code = (first - me * leaf_dev - base) * OFFS + (second - first)
    want = lax.broadcasted_iota(jnp.int32, (half * OFFS, slots), 0)
    hit = jnp.max(jnp.where(want == code, RATE, 0.0), axis=1, keepdims=True)
    mask[...] = jnp.broadcast_to(hit, mask.shape)
    acc[...] = jnp.zeros_like(acc)
    acc2[...] = jnp.zeros_like(acc2)

    @pl.when(jnp.logical_and(mine == 0, me > 0))
    def _():
        point_hop.start()

    def both(field, k):
        return jnp.concatenate([field[0, k], field[1, k]], axis=0)

    def stack(k, x):
        hi = x.astype(BF16)
        v2[k] = jnp.concatenate([hi, (x - hi.astype(F32)).astype(BF16)], axis=0)

    def add(into, k, x):
        into[0, k] += x[:cols]
        into[1, k] += x[cols:]

    rows = 2 * cols

    def tile(s):
        return [
            jnp.concatenate([tiles[s, p, h] for h in range(width // 128)], axis=1)
            for p in range(2)
        ]

    def columns(vi, hi, lo):
        x = dot(vi, hi, 1, 0)
        return x[:rows] + x[rows:] + dot(vi[:rows], lo, 1, 0)

    def products(i, into, make=None):
        vi = v2[i]
        row = jnp.zeros((2 * rows, width), F32)
        low = jnp.zeros((rows, width), F32)
        for o in range(OFFS):
            if make is not None:
                make(i, o)
            hi, lo = tile(i * OFFS + o)
            vj = v2[i + o]
            row = row + dot(vj, hi, 1, 1)
            low = low + dot(vj[:rows], lo, 1, 1)
            if o > 0:
                add(into, i + o, columns(vi, hi, lo))
        add(into, i, row[:rows] + row[rows:] + low)

    def first_products(i):
        vi = v2[i]
        for o in range(OFFS):
            hi, lo = tile(i * OFFS + o)
            x = columns(vi, hi, lo)
            if o > 0:
                add(acc2, i + o, x)
            else:
                diag[i] = x

    def last_products(i):
        row = jnp.zeros((2 * rows, width), F32)
        low = jnp.zeros((rows, width), F32)
        for o in range(1, OFFS):
            hi, lo = tile(i * OFFS + o)
            vj = v2[i + o]
            row = row + dot(vj, hi, 1, 1)
            low = low + dot(vj[:rows], lo, 1, 1)
        add(acc2, i, row[:rows] + row[rows:] + low + diag[i])

    def turn(i):
        turned = prow[i].T
        for c in range(3):
            pcb[c] = jnp.broadcast_to(turned[:, c : c + 1], (width, 128))

    def build(i, o):
        s = i * OFFS + o
        for h in range(width // 128):
            at = slice(h * 128, h * 128 + 128)
            listed = mask[pl.ds(s, 1), :]
            right = [
                jnp.broadcast_to(
                    jnp.where(listed > 0.0, prow[i + o, c : c + 1, at], prow[i, c : c + 1, at]),
                    (ROWS, 128),
                )
                for c in range(3)
            ]
            top = jnp.broadcast_to(listed, (ROWS, 128))
            for a in range(0, width, ROWS):
                dx = pcb[0, a : a + ROWS, :] - right[0]
                dy = pcb[1, a : a + ROWS, :] - right[1]
                dz = pcb[2, a : a + ROWS, :] - right[2]
                d2 = jnp.maximum(dx * dx + dy * dy + dz * dz, 1e-30)
                y = jnp.maximum(top - d2 * lax.rsqrt(d2), 0.0)
                y2 = y * y
                t = (y2 * y2) * (y2 + (LIN * y + CON)) * jnp.exp2(y)
                hi = t.astype(BF16)
                tiles[s, 0, h, a : a + ROWS, :] = hi
                tiles[s, 1, h, a : a + ROWS, :] = (t - hi.astype(F32)).astype(BF16)

    for k in range(half):
        d[mine, k] = own[base + k]

    @pl.when(mine == 0)
    def _():
        for k in range(half, span):
            d[0, k] = own[k]

    @pl.when(jnp.logical_and(mine == 1, me == n - 1))
    def _():
        d[:, pl.ds(half, REACH)] = jnp.zeros((2, REACH, cols, width), F32)
        prow[pl.ds(half, REACH)] = jnp.zeros((REACH, 8, width), F32)

    twin_hop.wait_recv()
    for k in range(half):
        stack(k, both(d, k))

    low_hop = hop(acc.at[:, pl.ds(0, REACH)], in_high, 5, low_leaf, twin)
    high_hop = hop(acc.at[:, pl.ds(half, REACH)], in_low, 6, high_leaf, twin)

    def first_pass(i, carry):
        @pl.when(jnp.logical_and(i == half - REACH, jnp.logical_and(mine == 1, me < n - 1)))
        def _():
            point_hop.wait_recv()

        @pl.when(i == half - REACH)
        def _():
            @pl.when(mine == 0)
            def _():
                ring_hop.wait_recv()

            @pl.when(jnp.logical_and(mine == 1, me < n - 1))
            def _():
                for k in range(2):
                    rim_in[k].wait_recv()

            for k in range(half, span):
                stack(k, both(d, k))

        turn(i)
        products(i, acc, build)

        @pl.when(jnp.logical_and(i == REACH - 1, has_low))
        def _():
            low_hop.start()

        return carry

    lax.fori_loop(0, half, first_pass, 0)

    @pl.when(has_high)
    def _():
        high_hop.start()

    @pl.when(jnp.logical_not(has_low))
    def _():
        in_low[...] = jnp.zeros_like(in_low)

    @pl.when(jnp.logical_not(has_high))
    def _():
        in_high[...] = jnp.zeros_like(in_high)

    def make_w(k, more):
        xs = []
        for r in range(2):
            x = acc[r, k]
            if more is not None:
                x = x + more[r]
            x = NORM * x - d[r, k]
            w[r, k] = x
            xs.append(x)
        stack(k, jnp.concatenate(xs, axis=0))

    for k in range(REACH, half):
        make_w(k, None)

    @pl.when(has_high)
    def _():
        low_hop.wait_recv()

    for k in range(half, span):
        make_w(k, [in_high[r, k - half] for r in range(2)])

    def whole_pass(i, carry):
        products(i, acc2)
        return carry

    lax.fori_loop(REACH, half, whole_pass, 0)
    early = jnp.zeros((rows, width), F32)
    for k in range(REACH, span):
        early = early + both(w, k) * both(acc2, k)

    @pl.when(has_low)
    def _():
        high_hop.wait_recv()

    for k in range(REACH):
        make_w(k, [in_low[r, k] for r in range(2)])

    far_hop = hop(w.at[other, pl.ds(0, half)], wfar, 7, me, twin)
    far_hop.start()
    give_hop = hop(acc2.at[other, pl.ds(0, half)], part.at[pl.ds(0, half)], 8, me, twin)
    give_rim = hop(acc2.at[other, pl.ds(half, REACH)], part.at[pl.ds(half, REACH)], 9, me, twin)
    next_even = hop(acc2.at[0, pl.ds(half, REACH)], part.at[pl.ds(half, REACH)], 9, after, even)
    next_odd = hop(acc2.at[1, pl.ds(half, REACH)], back, 10, after, even + 1)

    def first_half(t, carry):
        i = REACH - 1 - t
        first_products(i)

        @pl.when(jnp.logical_and(i == half - REACH, mine == 0))
        def _():
            give_rim.start()

        @pl.when(jnp.logical_and(i == half - REACH, jnp.logical_and(mine == 1, me < n - 1)))
        def _():
            next_even.start()
            next_odd.start()

        return carry

    lax.fori_loop(0, REACH, first_half, 0)

    def lanes(x):
        return x[:, :128] + x[:, 128:] if width == 256 else x

    sums = [jnp.zeros((rows, width), F32) for _ in range(4)]
    for k in range(span):
        wk = both(w, k)
        sums[3] = sums[3] + wk * both(acc2, k)
        if k < REACH:
            early = early - wk * diag[k]
        if k < half:
            dk = both(d, k)
            sums[0] = sums[0] + dk * dk
            sums[1] = sums[1] + dk * wk
            sums[2] = sums[2] + wk * wk
    sums[3] = 2.0 * sums[3] - early
    stacked = jnp.concatenate([lanes(x) for x in sums], axis=0)
    parts = three(stacked, 1)
    total = dot(jnp.full((8, parts.shape[1]), 1.0, BF16), parts, 1, 1)
    sum_out[...] = total[0:1]
    copies = []
    for slot, leaf, row in peers:
        copy = pltpu.make_async_remote_copy(
            src_ref=sum_out, dst_ref=sum_in.at[slot],
            send_sem=ssem.at[slot], recv_sem=rsem.at[slot],
            device_id={"leaf": leaf, "probe": row}, device_id_type=MESH,
        )
        copy.start()
        copies.append(copy)

    def last_half(i, carry):
        last_products(i)
        return carry

    lax.fori_loop(0, REACH, last_half, 0)
    give_hop.start()

    @pl.when(jnp.logical_and(mine == 0, me == 0))
    def _():
        part[pl.ds(half, REACH)] = jnp.zeros((REACH, cols, width), F32)

    @pl.when(jnp.logical_and(mine == 1, me == 0))
    def _():
        back[...] = jnp.zeros_like(back)

    @pl.when(mine == 0)
    def _():
        back[...] = acc2[0, pl.ds(half, REACH)]

    total = sum_out[...]
    for slot, copy in enumerate(copies):
        copy.wait_recv()
        total = total + sum_in[slot]
    seat = lax.broadcasted_iota(jnp.int32, (cols, 128), 1)
    line = lax.broadcasted_iota(jnp.int32, (cols, 128), 0) + mine * cols
    rr, dw, ww, wk = [
        jnp.sum(jnp.where(seat == line + q * rows, total, 0.0), axis=1, keepdims=True)
        for q in range(4)
    ]
    wz = NORM * wk - ww
    m = dw / rr
    alpha0 = rr / (SHIFT * rr + dw)
    uu = ww - m * dw
    tilt = alpha0 * uu / rr
    alpha1 = uu / (SHIFT * uu + (m * (m * dw - 2.0 * ww) + wz) - tilt * uu)
    e = alpha0 * (m + tilt)
    both_alpha = alpha0 * alpha1
    sol_d = alpha0 + alpha1 * e
    res_d = alpha0 * m - SHIFT * alpha1 * e
    res_w = -(alpha0 + alpha1 * e - SHIFT * both_alpha) - both_alpha
    res_z = both_alpha * NORM

    far_hop.wait_recv()
    give_hop.wait_recv()

    @pl.when(mine == 1)
    def _():
        give_rim.wait_recv()

    @pl.when(jnp.logical_and(mine == 0, me > 0))
    def _():
        next_even.wait_recv()

    @pl.when(jnp.logical_and(mine == 1, me > 0))
    def _():
        next_odd.wait_recv()

    def finish(l, dl, wl, zl):
        at = pl.ds(pl.multiple_of(l * width, width), width)
        sol_ref[:, at] = sol_d * dl - both_alpha * wl
        res_ref[:, at] = res_d * dl + res_w * wl + res_z * zl

    for k in range(half):
        near = acc2[mine, k]
        far = part[k]
        if k < REACH:
            near = near + part[half + k]
            far = far + back[k]
        finish(base + k, d[mine, k], w[mine, k], near)
        finish(twin_base + k, own[twin_base + k], wfar[k], far)

    for copy in copies:
        copy.wait_send()
    for copy in (twin_hop, far_hop, give_hop):
        copy.wait_send()

    @pl.when(mine == 1)
    def _():
        ring_hop.wait_send()

    @pl.when(mine == 0)
    def _():
        give_rim.wait_send()

    @pl.when(jnp.logical_and(mine == 0, me > 0))
    def _():
        point_hop.wait_send()

    @pl.when(me > 0)
    def _():
        rim_hop.wait_send()

    @pl.when(has_low)
    def _():
        low_hop.wait_send()

    @pl.when(has_high)
    def _():
        high_hop.wait_send()

    @pl.when(jnp.logical_and(mine == 1, me < n - 1))
    def _():
        next_even.wait_send()
        next_odd.wait_send()


def body(coords, site_order, leaf_pairs, pair_count, probes):
    n = lax.axis_size("leaf")
    leaf_dev, width = site_order.shape
    cols = probes.shape[0]
    half = leaf_dev // 2
    span = half + REACH
    slots_in = 2 * n - 1
    hbm = pl.BlockSpec(memory_space=pltpu.HBM)
    vmem = pl.BlockSpec(memory_space=pltpu.VMEM)
    field = functools.partial(pltpu.VMEM, dtype=F32)
    return pl.pallas_call(
        functools.partial(kernel, n),
        out_shape=(jax.ShapeDtypeStruct(probes.shape, F32),) * 2,
        in_specs=[hbm] * 4,
        out_specs=(vmem, vmem),
        scratch_shapes=[
            field(coords.shape),
            pltpu.VMEM(site_order.shape, jnp.int32),
            pltpu.VMEM(leaf_pairs.shape, jnp.int32),
            field((leaf_dev, cols, width)),
            field((8, leaf_dev * width)),
            field((span, 8, width)),
            field((3, width, 128)),
            field((half * OFFS, 128)),
            pltpu.VMEM((half * OFFS, 2, width // 128, width, 128), BF16),
            field((2, span, cols, width)),
            field((2, span, cols, width)),
            field((half, cols, width)),
            pltpu.VMEM((span, 4 * cols, width), BF16),
            field((2, span, cols, width)),
            field((2, span, cols, width)),
            field((2, REACH, cols, width)),
            field((2, REACH, cols, width)),
            field((span, cols, width)),
            field((REACH, cols, width)),
            field((REACH, 2 * cols, width)),
            field((1, 128)),
            field((slots_in, 1, 128)),
            pltpu.SemaphoreType.DMA((3 + leaf_dev,)),
            pltpu.SemaphoreType.DMA((slots_in,)),
            pltpu.SemaphoreType.DMA((slots_in,)),
            pltpu.SemaphoreType.DMA((11,)),
            pltpu.SemaphoreType.DMA((11,)),
        ],
        compiler_params=pltpu.CompilerParams(
            collective_id=0, has_side_effects=True, vmem_limit_bytes=67043328
        ),
    )(coords, site_order, leaf_pairs, probes)


def solution(mesh):
    in_specs = (P(None, "leaf"), P("leaf", None), P(None, "leaf"), P("leaf"), P("probe", "leaf"))
    out_specs = (P("probe", "leaf"), P("probe", "leaf"))
    return jax.shard_map(body, mesh=mesh, in_specs=in_specs, out_specs=out_specs, check_vma=False)
```

```python
import functools
import math

import jax
import jax.numpy as jnp
from jax import lax
from jax.experimental import pallas as pl
from jax.experimental.pallas import tpu as pltpu
from jax.sharding import PartitionSpec as P

REACH = 5
UNIT = 0.025
LENGTH = 0.12
NUGGET = 0.5
SHIFT = NUGGET + 1.0
TAPER = REACH * UNIT
GROW = math.sqrt(3.0) * TAPER / LENGTH
RATE = GROW / math.log(2.0)
QUAD = 4.0 * GROW
LIN = -(4.0 + 9.0 * GROW) * RATE / QUAD
CON = 5.0 * (1.0 + GROW) * RATE**2 / QUAD
NORM = QUAD * 2.0**-RATE / RATE**6
OFFS = REACH + 1
AHEAD = 1
ROWS = 32
MESH = pl.DeviceIdType.MESH
F32 = jnp.float32
BF16 = jnp.bfloat16


def dot(a, b, ca, cb):
    return lax.dot_general(a, b, (((ca,), (cb,)), ((), ())), preferred_element_type=F32)


def three(x, axis):
    hi = x.astype(BF16).astype(F32)
    mid = (x - hi).astype(BF16).astype(F32)
    return jnp.concatenate([hi, mid, x - hi - mid], axis=axis).astype(BF16)


def kernel(
    n, coords_hbm, order_hbm, pairs_hbm, probes_hbm, sol_ref, res_ref,
    cin, order, pairs, own, c8, prow, pcb, mask, tiles, d, w, wfar, v2, acc, acc2,
    in_edge, in_twin, part, back, diag, sum_out, sum_in, word, line_done, isem, ssem, rsem, hsend, hrecv,
):
    leaf_dev, width = order.shape
    cols = probes_hbm.shape[0]
    half = leaf_dev // 2
    span = half + REACH
    me = lax.axis_index("leaf")
    probe = lax.axis_index("probe")
    mine = lax.rem(probe, 2)
    other = 1 - mine
    even = probe - mine
    twin = even + other
    base = half * mine
    twin_base = half * other
    after = lax.rem(me + 1, n)
    before = lax.rem(me + n - 1, n)
    edge_leaf = jnp.where(mine == 0, before, after)
    has_edge = jnp.where(mine == 0, me > 0, me < n - 1)
    edge = half * mine
    inner = half * other

    peers = [(k - 1, lax.rem(me + k, n), probe) for k in range(1, n)]
    peers += [(n - 1 + k, lax.rem(me + k, n), twin) for k in range(n)]
    slots_in = len(peers)

    def load(src, dst, slot):
        return pltpu.make_async_copy(src, dst, isem.at[slot])

    loads = [
        load(coords_hbm, cin, 0), load(order_hbm, order, 1), load(pairs_hbm, pairs, 2),
    ]
    for l in range(leaf_dev):
        loads.append(load(probes_hbm.at[:, l * width : (l + 1) * width], own.at[l], 3 + l))
    for copy in loads:
        copy.start()
    barrier = pltpu.get_barrier_semaphore()
    def greet(sem, leaf, row):
        pl.semaphore_signal(
            sem, inc=1, device_id={"leaf": leaf, "probe": row}, device_id_type=MESH
        )

    greet(barrier, me, twin)

    @pl.when(me > 0)
    def _():
        greet(barrier, me - 1, probe)
        greet(barrier, me - 1, twin)

    @pl.when(me < n - 1)
    def _():
        greet(barrier, me + 1, probe)
        greet(barrier, me + 1, twin)

    steps = []
    while (1 << len(steps)) < n - 1:
        steps.append(1 << len(steps))

    def tell(j):
        @pl.when(me >= steps[j])
        def _():
            greet(word.at[2 * j], me - steps[j], probe)

        @pl.when(me + steps[j] < n)
        def _():
            greet(word.at[2 * j + 1], me + steps[j], probe)

    def hear(j):
        @pl.when(me + steps[j] < n)
        def _():
            pl.semaphore_wait(word.at[2 * j], 1)

        @pl.when(me >= steps[j])
        def _():
            pl.semaphore_wait(word.at[2 * j + 1], 1)

    def hop(src, dst, slot, leaf, row, landing=None):
        return pltpu.make_async_remote_copy(
            src_ref=src, dst_ref=dst, send_sem=hsend.at[slot],
            recv_sem=hrecv.at[slot if landing is None else landing],
            device_id={"leaf": leaf, "probe": row}, device_id_type=MESH,
        )

    for copy in loads[3:]:
        copy.wait()
    near = jnp.where(me > 0, 2, 0) + jnp.where(me < n - 1, 2, 0)
    pl.semaphore_wait(barrier, 1 + near)
    tell(0)

    point_hop = hop(prow.at[pl.ds(0, REACH)], prow.at[pl.ds(half, REACH)], 0, before, twin)
    rim_hop = hop(own.at[pl.ds(0, REACH)], d.at[mine, pl.ds(half, REACH)], 1, before, even + 1, 1 + mine)
    rim_in = [
        hop(own.at[pl.ds(0, REACH)], d.at[k, pl.ds(half, REACH)], 1, before, even + 1, 1 + k)
        for k in range(2)
    ]
    twin_hop = hop(own.at[pl.ds(twin_base, half)], d.at[mine, pl.ds(0, half)], 3, me, twin)
    ring_hop = hop(own.at[pl.ds(half, REACH)], d.at[mine, pl.ds(half, REACH)], 4, me, twin)
    twin_hop.start()

    @pl.when(mine == 1)
    def _():
        ring_hop.start()

    @pl.when(me > 0)
    def _():
        rim_hop.start()

    place = lax.broadcasted_iota(jnp.int32, (width, width), 0)
    for copy in loads[:3]:
        copy.wait()
    c8[...] = jnp.zeros_like(c8)
    c8[0:3, :] = cin[...] * (RATE / TAPER)

    def gather(k):
        x = c8[:, pl.ds(pl.multiple_of((base + k) * width, width), width)]
        parts = three(x, 0)
        onehot = jnp.where(place == order[pl.ds(base + k, 1), :], 1.0, 0.0).astype(BF16)
        got = dot(parts, onehot, 1, 0)
        prow[k] = got[0:8] + got[8:16] + got[16:24]

    for k in range(half):
        gather(k)

    @pl.when(mine == 0)
    def _():
        for k in range(half, span):
            gather(k)

    slots = pairs.shape[1]
    first = pairs[0:1, :]
    second = pairs[1:2, :]
    code = (first - me * leaf_dev - base) * OFFS + (second - first)
    want = lax.broadcasted_iota(jnp.int32, (half * OFFS, slots), 0)
    hit = jnp.max(jnp.where(want == code, RATE, 0.0), axis=1, keepdims=True)
    mask[...] = jnp.broadcast_to(hit, mask.shape)
    acc[...] = jnp.zeros_like(acc)
    acc2[...] = jnp.zeros_like(acc2)

    @pl.when(jnp.logical_and(mine == 0, me > 0))
    def _():
        point_hop.start()

    def both(field, k):
        return jnp.concatenate([field[0, k], field[1, k]], axis=0)

    def stack(k, x):
        hi = x.astype(BF16)
        v2[k] = jnp.concatenate([hi, (x - hi.astype(F32)).astype(BF16)], axis=0)

    def add(into, k, x):
        into[0, k] += x[:cols]
        into[1, k] += x[cols:]

    rows = 2 * cols

    def tile(s):
        return [
            jnp.concatenate([tiles[s, p, h] for h in range(width // 128)], axis=1)
            for p in range(2)
        ]

    def columns(vi, hi, lo):
        x = dot(vi, hi, 1, 0)
        return x[:rows] + x[rows:] + dot(vi[:rows], lo, 1, 0)

    def products(i, into, make):
        vi = v2[i]
        cut = width // 2
        row = [jnp.zeros((cut, 2 * rows), F32) for _ in range(2)]
        for o in range(OFFS):
            make(i, o)
            hi, lo = tile(i * OFFS + o)
            vj = v2[i + o]
            for q in range(2):
                at = slice(q * cut, q * cut + cut)
                row[q] = row[q] + dot(hi[at], vj, 1, 1) + dot(lo[at], vj, 1, 1)
            if o > 0:
                add(into, i + o, columns(vi, hi, lo))
        row = jnp.concatenate([x.T for x in row], axis=1)
        add(into, i, row[:rows] + row[rows:])

    def first_products(i):
        vi = v2[i]
        for o in range(OFFS):
            hi, lo = tile(i * OFFS + o)
            x = columns(vi, hi, lo)
            if o > 0:
                add(acc2, i + o, x)
            else:
                diag[i] = x

    def last_products(i):
        row = jnp.zeros((2 * rows, width), F32)
        low = jnp.zeros((rows, width), F32)
        for o in range(1, OFFS):
            hi, lo = tile(i * OFFS + o)
            vj = v2[i + o]
            row = row + dot(vj, hi, 1, 1)
            low = low + dot(vj[:rows], lo, 1, 1)
        add(acc2, i, row[:rows] + row[rows:] + low + diag[i])

    def turn(i):
        turned = prow[i].T
        for c in range(3):
            pcb[c] = jnp.broadcast_to(turned[:, c : c + 1], (width, 128))

    def build(i, o):
        s = i * OFFS + o
        for h in range(width // 128):
            at = slice(h * 128, h * 128 + 128)
            listed = mask[pl.ds(s, 1), :]
            right = [
                jnp.broadcast_to(
                    jnp.where(listed > 0.0, prow[i + o, c : c + 1, at], prow[i, c : c + 1, at]),
                    (ROWS, 128),
                )
                for c in range(3)
            ]
            top = jnp.broadcast_to(listed, (ROWS, 128))
            for a in range(0, width, ROWS):
                dx = pcb[0, a : a + ROWS, :] - right[0]
                dy = pcb[1, a : a + ROWS, :] - right[1]
                dz = pcb[2, a : a + ROWS, :] - right[2]
                d2 = jnp.maximum(dx * dx + dy * dy + dz * dz, 1e-30)
                y = jnp.maximum(top - d2 * lax.rsqrt(d2), 0.0)
                y2 = y * y
                t = (y2 * y2) * (y2 + (LIN * y + CON)) * jnp.exp2(y)
                hi = t.astype(BF16)
                tiles[s, 0, h, a : a + ROWS, :] = hi
                tiles[s, 1, h, a : a + ROWS, :] = (t - hi.astype(F32)).astype(BF16)

    for k in range(half):
        d[mine, k] = own[base + k]

    @pl.when(mine == 0)
    def _():
        for k in range(half, span):
            d[0, k] = own[k]

    @pl.when(jnp.logical_and(mine == 1, me == n - 1))
    def _():
        d[:, pl.ds(half, REACH)] = jnp.zeros((2, REACH, cols, width), F32)
        prow[pl.ds(half, REACH)] = jnp.zeros((REACH, 8, width), F32)

    twin_hop.wait_recv()
    for k in range(half):
        stack(k, both(d, k))

    edge_hop = hop(acc.at[:, pl.ds(edge, REACH)], in_edge, 5, edge_leaf, twin)
    inner_hop = hop(acc.at[:, pl.ds(inner, REACH)], in_twin, 6, me, twin)
    lag = half - REACH

    def first_pass(t, carry):
        i = jnp.where(
            mine == 0, t, jnp.where(t < AHEAD, t, jnp.where(t < AHEAD + REACH, t + lag - AHEAD, t - REACH))
        )

        @pl.when(i == lag)
        def _():
            @pl.when(mine == 0)
            def _():
                ring_hop.wait_recv()

            @pl.when(jnp.logical_and(mine == 1, me < n - 1))
            def _():
                point_hop.wait_recv()
                for k in range(2):
                    rim_in[k].wait_recv()

            for k in range(half, span):
                stack(k, both(d, k))

        for j in range(len(steps) - 1):
            @pl.when(t == 2 * j + 1)
            def _(j=j):
                hear(j)
                tell(j + 1)

        turn(i)
        products(i, acc, build)

        @pl.when(jnp.logical_and(t == REACH - 1 + AHEAD * mine, has_edge))
        def _():
            edge_hop.start()

        return carry

    lax.fori_loop(0, half, first_pass, 0)
    inner_hop.start()
    for j in range(half // 2, len(steps) - 1):
        hear(j)
        tell(j + 1)

    @pl.when(jnp.logical_not(has_edge))
    def _():
        in_edge[...] = jnp.zeros_like(in_edge)

    def make_w(k, more):
        xs = []
        for r in range(2):
            x = acc[r, k]
            if more is not None:
                x = x + more[r]
            x = NORM * x - d[r, k]
            w[r, k] = x
            xs.append(x)
        stack(k, jnp.concatenate(xs, axis=0))

    for k in range(REACH, half):
        make_w(k, None)

    @pl.when(has_edge)
    def _():
        edge_hop.wait_recv()

    for k in range(REACH):
        make_w(edge + k, [in_edge[r, k] for r in range(2)])

    def outer_columns(t, carry):
        first_products(t + REACH * mine)
        return carry

    lax.fori_loop(0, lag, outer_columns, 0)
    inner_hop.wait_recv()
    for k in range(REACH):
        make_w(inner + k, [in_twin[r, k] for r in range(2)])

    far_hop = hop(w.at[other, pl.ds(0, half)], wfar, 7, me, twin)
    far_hop.start()
    give_hop = hop(acc2.at[other, pl.ds(0, half)], part.at[pl.ds(0, half)], 8, me, twin)
    give_rim = hop(acc2.at[other, pl.ds(half, REACH)], part.at[pl.ds(half, REACH)], 9, me, twin)
    next_even = hop(acc2.at[0, pl.ds(half, REACH)], part.at[pl.ds(half, REACH)], 9, after, even)
    next_odd = hop(acc2.at[1, pl.ds(half, REACH)], back, 10, after, even + 1)

    left = lag * other

    def first_half(t, carry):
        i = left + REACH - 1 - t
        first_products(i)

        @pl.when(jnp.logical_and(i == lag, mine == 0))
        def _():
            give_rim.start()

        @pl.when(jnp.logical_and(i == lag, jnp.logical_and(mine == 1, me < n - 1)))
        def _():
            next_even.start()
            next_odd.start()

        return carry

    lax.fori_loop(0, REACH, first_half, 0)

    def lanes(x):
        return x[:, :128] + x[:, 128:] if width == 256 else x

    sums = [jnp.zeros((rows, width), F32) for _ in range(4)]
    own_part = jnp.zeros((rows, width), F32)
    for k in range(span):
        wk = both(w, k)
        sums[3] = sums[3] + wk * both(acc2, k)
        if k < half:
            own_part = own_part + wk * diag[k]
        if k < half:
            dk = both(d, k)
            sums[0] = sums[0] + dk * dk
            sums[1] = sums[1] + dk * wk
            sums[2] = sums[2] + wk * wk
    sums[3] = 2.0 * sums[3] + own_part
    stacked = jnp.concatenate([lanes(x) for x in sums], axis=0)
    parts = three(stacked, 1)
    total = dot(jnp.full((8, parts.shape[1]), 1.0, BF16), parts, 1, 1)
    sum_out[...] = total[0:1]
    hear(len(steps) - 1)
    greet(line_done, me, twin)
    pl.semaphore_wait(line_done, 1)
    copies = []
    for slot, leaf, row in peers:
        copy = pltpu.make_async_remote_copy(
            src_ref=sum_out, dst_ref=sum_in.at[slot],
            send_sem=ssem.at[slot], recv_sem=rsem.at[slot],
            device_id={"leaf": leaf, "probe": row}, device_id_type=MESH,
        )
        copy.start()
        copies.append(copy)

    def last_half(i, carry):
        last_products(i)
        return carry

    lax.fori_loop(0, half, last_half, 0)
    give_hop.start()

    @pl.when(jnp.logical_and(mine == 0, me == 0))
    def _():
        part[pl.ds(half, REACH)] = jnp.zeros((REACH, cols, width), F32)

    @pl.when(jnp.logical_and(mine == 1, me == 0))
    def _():
        back[...] = jnp.zeros_like(back)

    @pl.when(mine == 0)
    def _():
        back[...] = acc2[0, pl.ds(half, REACH)]

    total = sum_out[...]
    for slot, copy in enumerate(copies):
        copy.wait_recv()
        total = total + sum_in[slot]
    seat = lax.broadcasted_iota(jnp.int32, (cols, 128), 1)
    line = lax.broadcasted_iota(jnp.int32, (cols, 128), 0) + mine * cols
    rr, dw, ww, wk = [
        jnp.sum(jnp.where(seat == line + q * rows, total, 0.0), axis=1, keepdims=True)
        for q in range(4)
    ]
    wz = NORM * wk - ww
    m = dw / rr
    alpha0 = rr / (SHIFT * rr + dw)
    uu = ww - m * dw
    tilt = alpha0 * uu / rr
    alpha1 = uu / (SHIFT * uu + (m * (m * dw - 2.0 * ww) + wz) - tilt * uu)
    e = alpha0 * (m + tilt)
    both_alpha = alpha0 * alpha1
    sol_d = alpha0 + alpha1 * e
    res_d = alpha0 * m - SHIFT * alpha1 * e
    res_w = -(alpha0 + alpha1 * e - SHIFT * both_alpha) - both_alpha
    res_z = both_alpha * NORM

    far_hop.wait_recv()
    give_hop.wait_recv()

    @pl.when(mine == 1)
    def _():
        give_rim.wait_recv()

    @pl.when(jnp.logical_and(mine == 0, me > 0))
    def _():
        next_even.wait_recv()

    @pl.when(jnp.logical_and(mine == 1, me > 0))
    def _():
        next_odd.wait_recv()

    def finish(l, dl, wl, zl):
        at = pl.ds(pl.multiple_of(l * width, width), width)
        sol_ref[:, at] = sol_d * dl - both_alpha * wl
        res_ref[:, at] = res_d * dl + res_w * wl + res_z * zl

    for k in range(half):
        near = acc2[mine, k]
        far = part[k]
        if k < REACH:
            near = near + part[half + k]
            far = far + back[k]
        finish(base + k, d[mine, k], w[mine, k], near)
        finish(twin_base + k, own[twin_base + k], wfar[k], far)

    for copy in copies:
        copy.wait_send()
    for copy in (twin_hop, inner_hop, far_hop, give_hop):
        copy.wait_send()

    @pl.when(mine == 1)
    def _():
        ring_hop.wait_send()

    @pl.when(mine == 0)
    def _():
        give_rim.wait_send()

    @pl.when(jnp.logical_and(mine == 0, me > 0))
    def _():
        point_hop.wait_send()

    @pl.when(me > 0)
    def _():
        rim_hop.wait_send()

    @pl.when(has_edge)
    def _():
        edge_hop.wait_send()

    @pl.when(jnp.logical_and(mine == 1, me < n - 1))
    def _():
        next_even.wait_send()
        next_odd.wait_send()


def body(coords, site_order, leaf_pairs, pair_count, probes):
    arrays = (coords, site_order, leaf_pairs, probes)
    n = lax.axis_size("leaf")
    leaf_dev, width = site_order.shape
    cols = probes.shape[0]
    half = leaf_dev // 2
    span = half + REACH
    slots_in = 2 * n - 1
    hbm = pl.BlockSpec(memory_space=pltpu.HBM)
    vmem = pl.BlockSpec(memory_space=pltpu.VMEM)
    field = functools.partial(pltpu.VMEM, dtype=F32)
    return pl.pallas_call(
        functools.partial(kernel, n),
        out_shape=(jax.ShapeDtypeStruct(probes.shape, F32),) * 2,
        in_specs=[hbm] * 4,
        out_specs=(vmem, vmem),
        scratch_shapes=[
            field(coords.shape),
            pltpu.VMEM(site_order.shape, jnp.int32),
            pltpu.VMEM(leaf_pairs.shape, jnp.int32),
            field((leaf_dev, cols, width)),
            field((8, leaf_dev * width)),
            field((span, 8, width)),
            field((3, width, 128)),
            field((half * OFFS, 128)),
            pltpu.VMEM((half * OFFS, 2, width // 128, width, 128), BF16),
            field((2, span, cols, width)),
            field((2, span, cols, width)),
            field((half, cols, width)),
            pltpu.VMEM((span, 4 * cols, width), BF16),
            field((2, span, cols, width)),
            field((2, span, cols, width)),
            field((2, REACH, cols, width)),
            field((2, REACH, cols, width)),
            field((span, cols, width)),
            field((REACH, cols, width)),
            field((half, 2 * cols, width)),
            field((1, 128)),
            field((slots_in, 1, 128)),
            pltpu.SemaphoreType.REGULAR((2 * n.bit_length(),)),
            pltpu.SemaphoreType.REGULAR,
            pltpu.SemaphoreType.DMA((3 + leaf_dev,)),
            pltpu.SemaphoreType.DMA((slots_in,)),
            pltpu.SemaphoreType.DMA((slots_in,)),
            pltpu.SemaphoreType.DMA((11,)),
            pltpu.SemaphoreType.DMA((11,)),
        ],
        compiler_params=pltpu.CompilerParams(
            collective_id=0, has_side_effects=True, vmem_limit_bytes=48 * 2**20
        ),
    )(*[pltpu.with_memory_space_constraint(x, pltpu.HBM) for x in arrays])


def solution(mesh):
    in_specs = (P(None, "leaf"), P("leaf", None), P(None, "leaf"), P("leaf"), P("probe", "leaf"))
    out_specs = (P("probe", "leaf"), P("probe", "leaf"))
    return jax.shard_map(body, mesh=mesh, in_specs=in_specs, out_specs=out_specs, check_vma=False)
```

```python
import functools
import math

import jax
import jax.numpy as jnp
from jax import lax
from jax.experimental import pallas as pl
from jax.experimental.pallas import tpu as pltpu
from jax.sharding import PartitionSpec as P

REACH = 5
UNIT = 0.025
LENGTH = 0.12
NUGGET = 0.5
SHIFT = NUGGET + 1.0
TAPER = REACH * UNIT
GROW = math.sqrt(3.0) * TAPER / LENGTH
RATE = GROW / math.log(2.0)
QUAD = 4.0 * GROW
LIN = -(4.0 + 9.0 * GROW) * RATE / QUAD
CON = 5.0 * (1.0 + GROW) * RATE**2 / QUAD
NORM = QUAD * 2.0**-RATE / RATE**6
OFFS = REACH + 1
AHEAD = 1
ROWS = 32
MESH = pl.DeviceIdType.MESH
F32 = jnp.float32
BF16 = jnp.bfloat16


def dot(a, b, ca, cb):
    return lax.dot_general(a, b, (((ca,), (cb,)), ((), ())), preferred_element_type=F32)


def three(x, axis):
    hi = x.astype(BF16).astype(F32)
    mid = (x - hi).astype(BF16).astype(F32)
    return jnp.concatenate([hi, mid, x - hi - mid], axis=axis).astype(BF16)


def kernel(
    n, coords_hbm, order_hbm, pairs_hbm, probes_hbm, out_ref,
    cin, order, pairs, own, c8, prow, pcb, mask, tiles, d, w, wfar, v2, acc, acc2,
    in_edge, in_twin, part, back, diag, sum_out, sum_in, word, line_done, isem, ssem, rsem, hsend, hrecv, esend, erecv,
):
    leaf_dev, width = order.shape
    cols = probes_hbm.shape[0]
    half = leaf_dev // 2
    span = half + REACH
    me = lax.axis_index("leaf")
    probe = lax.axis_index("probe")
    mine = lax.rem(probe, 2)
    other = 1 - mine
    even = probe - mine
    twin = even + other
    base = half * mine
    twin_base = half * other
    after = lax.rem(me + 1, n)
    before = lax.rem(me + n - 1, n)
    edge_leaf = jnp.where(mine == 0, before, after)
    has_edge = jnp.where(mine == 0, me > 0, me < n - 1)
    edge = half * mine
    inner = half * other

    peers = [(k - 1, lax.rem(me + k, n), probe) for k in range(1, n)]
    peers += [(n - 1 + k, lax.rem(me + k, n), twin) for k in range(n)]
    slots_in = len(peers)

    def load(src, dst, slot):
        return pltpu.make_async_copy(src, dst, isem.at[slot])

    loads = [
        load(coords_hbm, cin, 0), load(order_hbm, order, 1), load(pairs_hbm, pairs, 2),
    ]
    def leaves(ref, first, count):
        return ref.at[:, pl.ds(pl.multiple_of(first * width, width), count * width)]

    def into_d(r, first, count):
        return d.at[r, :, first * width : (first + count) * width]

    loads.append(load(leaves(probes_hbm, base, half), into_d(mine, 0, half), 3))
    loads.append(load(leaves(probes_hbm, twin_base, half), own, 4))
    ring_load = load(leaves(probes_hbm, half, REACH), into_d(0, half, REACH), 5)
    for copy in loads:
        copy.start()

    @pl.when(mine == 0)
    def _():
        ring_load.start()

    barrier = pltpu.get_barrier_semaphore()
    def greet(sem, leaf, row):
        pl.semaphore_signal(
            sem, inc=1, device_id={"leaf": leaf, "probe": row}, device_id_type=MESH
        )

    greet(barrier, me, twin)

    @pl.when(me < n - 1)
    def _():
        greet(barrier, me + 1, probe)
        greet(barrier, me + 1, twin)

    steps = [1]
    while (1 << len(steps) - 1) < n - 1:
        steps.append(1 << len(steps) - 1)

    def tell(j):
        @pl.when(me >= steps[j])
        def _():
            greet(word.at[2 * j], me - steps[j], probe)

        if j > 0:

            @pl.when(me + steps[j] < n)
            def _():
                greet(word.at[2 * j + 1], me + steps[j], probe)

    def hear(j):
        @pl.when(me + steps[j] < n)
        def _():
            pl.semaphore_wait(word.at[2 * j], 1)

        if j > 0:

            @pl.when(me >= steps[j])
            def _():
                pl.semaphore_wait(word.at[2 * j + 1], 1)

    def hop(src, dst, slot, leaf, row, landing=None):
        return pltpu.make_async_remote_copy(
            src_ref=src, dst_ref=dst, send_sem=hsend.at[slot],
            recv_sem=hrecv.at[slot if landing is None else landing],
            device_id={"leaf": leaf, "probe": row}, device_id_type=MESH,
        )

    pl.semaphore_wait(barrier, 1 + jnp.where(me > 0, 2, 0))
    tell(0)

    point_hop = hop(prow.at[pl.ds(0, REACH)], prow.at[pl.ds(half, REACH)], 0, before, twin)
    rim_hop = hop(leaves(probes_hbm, 0, REACH), into_d(mine, half, REACH), 1, before, even + 1, 1 + mine)
    rim_in = [
        hop(leaves(probes_hbm, 0, REACH), into_d(k, half, REACH), 1, before, even + 1, 1 + k)
        for k in range(2)
    ]
    twin_hop = hop(leaves(probes_hbm, twin_base, half), into_d(mine, 0, half), 3, me, twin)
    ring_hop = hop(leaves(probes_hbm, half, REACH), into_d(mine, half, REACH), 4, me, twin)
    twin_hop.start()

    @pl.when(mine == 1)
    def _():
        ring_hop.start()

    @pl.when(me > 0)
    def _():
        rim_hop.start()

    place = lax.broadcasted_iota(jnp.int32, (width, width), 0)
    for copy in loads[:3]:
        copy.wait()
    c8[...] = jnp.zeros_like(c8)
    c8[0:3, :] = cin[...] * (RATE / TAPER)

    def gather(k):
        x = c8[:, pl.ds(pl.multiple_of((base + k) * width, width), width)]
        parts = three(x, 0)
        onehot = jnp.where(place == order[pl.ds(base + k, 1), :], 1.0, 0.0).astype(BF16)
        got = dot(parts, onehot, 1, 0)
        prow[k] = got[0:8] + got[8:16] + got[16:24]

    for k in range(half):
        gather(k)

    @pl.when(mine == 0)
    def _():
        for k in range(half, span):
            gather(k)

    slots = pairs.shape[1]
    first = pairs[0:1, :]
    second = pairs[1:2, :]
    code = (first - me * leaf_dev - base) * OFFS + (second - first)
    want = lax.broadcasted_iota(jnp.int32, (half * OFFS, slots), 0)
    hit = jnp.max(jnp.where(want == code, RATE, 0.0), axis=1, keepdims=True)
    mask[...] = jnp.broadcast_to(hit, mask.shape)
    acc[...] = jnp.zeros_like(acc)
    acc2[...] = jnp.zeros_like(acc2)

    @pl.when(jnp.logical_and(mine == 0, me > 0))
    def _():
        point_hop.start()

    def both(field, k):
        return jnp.concatenate([field[0, k], field[1, k]], axis=0)

    def probe_rows(r, k):
        return d[r, :, pl.ds(pl.multiple_of(k * width, width), width)]

    def both_probes(k):
        return jnp.concatenate([probe_rows(0, k), probe_rows(1, k)], axis=0)

    def stack(k, x):
        hi = x.astype(BF16)
        v2[k] = jnp.concatenate([hi, (x - hi.astype(F32)).astype(BF16)], axis=0)

    def add(into, k, x):
        into[0, k] += x[:cols]
        into[1, k] += x[cols:]

    rows = 2 * cols

    def tile(s):
        return [
            jnp.concatenate([tiles[s, p, h] for h in range(width // 128)], axis=1)
            for p in range(2)
        ]

    def columns(vi, hi, lo):
        x = dot(vi, hi, 1, 0)
        return x[:rows] + x[rows:] + dot(vi[:rows], lo, 1, 0)

    def products(i, into, make):
        vi = v2[i]
        cut = width // 2
        row = [jnp.zeros((cut, 2 * rows), F32) for _ in range(2)]
        for o in range(OFFS):
            make(i, o)
            hi, lo = tile(i * OFFS + o)
            vj = v2[i + o]
            for q in range(2):
                at = slice(q * cut, q * cut + cut)
                row[q] = row[q] + dot(hi[at], vj, 1, 1) + dot(lo[at], vj, 1, 1)
            if o > 0:
                add(into, i + o, columns(vi, hi, lo))
        row = jnp.concatenate([x.T for x in row], axis=1)
        add(into, i, row[:rows] + row[rows:])

    def first_products(i):
        vi = v2[i]
        for o in range(OFFS):
            hi, lo = tile(i * OFFS + o)
            x = columns(vi, hi, lo)
            if o > 0:
                add(acc2, i + o, x)
            else:
                diag[i] = x

    def last_products(i):
        row = jnp.zeros((2 * rows, width), F32)
        low = jnp.zeros((rows, width), F32)
        for o in range(1, OFFS):
            hi, lo = tile(i * OFFS + o)
            vj = v2[i + o]
            row = row + dot(vj, hi, 1, 1)
            low = low + dot(vj[:rows], lo, 1, 1)
        add(acc2, i, row[:rows] + row[rows:] + low + diag[i])

    def turn(i):
        turned = prow[i].T
        for c in range(3):
            pcb[c] = jnp.broadcast_to(turned[:, c : c + 1], (width, 128))

    def build(i, o):
        s = i * OFFS + o
        for h in range(width // 128):
            at = slice(h * 128, h * 128 + 128)
            listed = mask[pl.ds(s, 1), :]
            right = [
                jnp.broadcast_to(
                    jnp.where(listed > 0.0, prow[i + o, c : c + 1, at], prow[i, c : c + 1, at]),
                    (ROWS, 128),
                )
                for c in range(3)
            ]
            top = jnp.broadcast_to(listed, (ROWS, 128))
            for a in range(0, width if o > 0 else at.stop, ROWS):
                dx = pcb[0, a : a + ROWS, :] - right[0]
                dy = pcb[1, a : a + ROWS, :] - right[1]
                dz = pcb[2, a : a + ROWS, :] - right[2]
                d2 = jnp.maximum(dx * dx + dy * dy + dz * dz, 1e-30)
                y = jnp.maximum(top - d2 * lax.rsqrt(d2), 0.0)
                y2 = y * y
                t = (y2 * y2) * (y2 + (LIN * y + CON)) * jnp.exp2(y)
                hi = t.astype(BF16)
                tiles[s, 0, h, a : a + ROWS, :] = hi
                tiles[s, 1, h, a : a + ROWS, :] = (t - hi.astype(F32)).astype(BF16)
            if o == 0:
                for p in range(2):
                    for g in range(h):
                        block = tiles[s, p, h, g * 128 : g * 128 + 128, :]
                        tiles[s, p, g, h * 128 : h * 128 + 128, :] = block.T

    for copy in loads[3:]:
        copy.wait()

    @pl.when(mine == 0)
    def _():
        ring_load.wait()

    @pl.when(jnp.logical_and(mine == 1, me == n - 1))
    def _():
        d[:, :, half * width :] = jnp.zeros((2, cols, REACH * width), F32)
        prow[pl.ds(half, REACH)] = jnp.zeros((REACH, 8, width), F32)

    twin_hop.wait_recv()
    for k in range(half):
        stack(k, both_probes(k))

    edge_hops = []
    for j in range(REACH):
        seat = jnp.where(mine == 0, j, REACH - 1 - j)
        edge_hops.append(
            pltpu.make_async_remote_copy(
                src_ref=acc.at[:, edge + seat], dst_ref=in_edge.at[:, seat],
                send_sem=esend.at[seat], recv_sem=erecv.at[seat],
                device_id={"leaf": edge_leaf, "probe": twin}, device_id_type=MESH,
            )
        )
    inner_hop = hop(acc.at[:, pl.ds(inner, REACH)], in_twin, 6, me, twin)
    lag = half - REACH

    def leaf_at(t):
        late = jnp.where(t < AHEAD + REACH, half - 1 + AHEAD - t, t - REACH)
        return jnp.where(mine == 0, t, jnp.where(t < AHEAD, t, late))

    turn(0)

    def first_pass(t, carry):
        i = leaf_at(t)

        @pl.when(t == jnp.where(mine == 0, lag, AHEAD))
        def _():
            @pl.when(mine == 0)
            def _():
                ring_hop.wait_recv()

            @pl.when(jnp.logical_and(mine == 1, me < n - 1))
            def _():
                point_hop.wait_recv()
                for k in range(2):
                    rim_in[k].wait_recv()

            for k in range(half, span):
                stack(k, both_probes(k))

        for j in range(len(steps) - 1):
            @pl.when(t == j + 2)
            def _(j=j):
                hear(j)
                tell(j + 1)

        products(i, acc, build)
        turn(leaf_at(jnp.minimum(t + 1, half - 1)))

        for j in range(REACH):

            @pl.when(jnp.logical_and(t == j + AHEAD * mine, has_edge))
            def _(j=j):
                edge_hops[j].start()

        return carry

    lax.fori_loop(0, half, first_pass, 0)
    inner_hop.start()
    for j in range(half - 2, len(steps) - 1):
        hear(j)
        tell(j + 1)

    @pl.when(jnp.logical_not(has_edge))
    def _():
        in_edge[...] = jnp.zeros_like(in_edge)

    def make_w(k, more):
        xs = []
        for r in range(2):
            x = acc[r, k]
            if more is not None:
                x = x + more[r]
            x = NORM * x - probe_rows(r, k)
            w[r, k] = x
            xs.append(x)
        stack(k, jnp.concatenate(xs, axis=0))

    for k in range(REACH, half):
        make_w(k, None)

    @pl.when(has_edge)
    def _():
        for copy in edge_hops:
            copy.wait_recv()

    for k in range(REACH):
        make_w(edge + k, [in_edge[r, k] for r in range(2)])

    def outer_columns(t, carry):
        first_products(t + REACH * mine)
        return carry

    lax.fori_loop(0, lag, outer_columns, 0)
    inner_hop.wait_recv()
    for k in range(REACH):
        make_w(inner + k, [in_twin[r, k] for r in range(2)])

    far_hop = hop(w.at[other, pl.ds(0, half)], wfar, 7, me, twin)
    far_hop.start()
    give_hop = hop(acc2.at[other, pl.ds(0, half)], part.at[pl.ds(0, half)], 8, me, twin)
    give_rim = hop(acc2.at[other, pl.ds(half, REACH)], part.at[pl.ds(half, REACH)], 9, me, twin)
    next_even = hop(acc2.at[0, pl.ds(half, REACH)], part.at[pl.ds(half, REACH)], 9, after, even)
    next_odd = hop(acc2.at[1, pl.ds(half, REACH)], back, 10, after, even + 1)

    left = lag * other

    def first_half(t, carry):
        i = left + REACH - 1 - t
        first_products(i)

        @pl.when(jnp.logical_and(i == lag, mine == 0))
        def _():
            give_rim.start()

        @pl.when(jnp.logical_and(i == lag, jnp.logical_and(mine == 1, me < n - 1)))
        def _():
            next_even.start()
            next_odd.start()

        return carry

    hear(len(steps) - 1)
    greet(line_done, me, twin)
    lax.fori_loop(0, REACH, first_half, 0)

    def lanes(x):
        return x[:, :128] + x[:, 128:] if width == 256 else x

    sums = [jnp.zeros((rows, width), F32) for _ in range(4)]
    own_part = jnp.zeros((rows, width), F32)
    for k in range(span):
        wk = both(w, k)
        sums[3] = sums[3] + wk * both(acc2, k)
        if k < half:
            own_part = own_part + wk * diag[k]
        if k < half:
            dk = both_probes(k)
            sums[0] = sums[0] + dk * dk
            sums[1] = sums[1] + dk * wk
            sums[2] = sums[2] + wk * wk
    sums[3] = 2.0 * sums[3] + own_part
    stacked = jnp.concatenate([lanes(x) for x in sums], axis=0)
    parts = three(stacked, 1)
    total = dot(jnp.full((8, parts.shape[1]), 1.0, BF16), parts, 1, 1)
    sum_out[...] = total[0:1]
    pl.semaphore_wait(line_done, 1)
    copies = []
    for slot, leaf, row in peers:
        copy = pltpu.make_async_remote_copy(
            src_ref=sum_out, dst_ref=sum_in.at[slot],
            send_sem=ssem.at[slot], recv_sem=rsem.at[slot],
            device_id={"leaf": leaf, "probe": row}, device_id_type=MESH,
        )
        copy.start()
        copies.append(copy)

    def last_half(i, carry):
        last_products(i)
        return carry

    lax.fori_loop(0, half, last_half, 0)
    give_hop.start()

    @pl.when(jnp.logical_and(mine == 0, me == 0))
    def _():
        part[pl.ds(half, REACH)] = jnp.zeros((REACH, cols, width), F32)

    @pl.when(jnp.logical_and(mine == 1, me == 0))
    def _():
        back[...] = jnp.zeros_like(back)

    @pl.when(mine == 0)
    def _():
        back[...] = acc2[0, pl.ds(half, REACH)]

    total = sum_out[...]
    for slot, copy in enumerate(copies):
        copy.wait_recv()
        total = total + sum_in[slot]
    column = lax.broadcasted_iota(jnp.int32, (cols, 128), 1)
    line = lax.broadcasted_iota(jnp.int32, (cols, 128), 0) + mine * cols
    rr, dw, ww, wk = [
        jnp.sum(jnp.where(column == line + q * rows, total, 0.0), axis=1, keepdims=True)
        for q in range(4)
    ]
    wz = NORM * wk - ww
    m = dw / rr
    alpha0 = rr / (SHIFT * rr + dw)
    uu = ww - m * dw
    tilt = alpha0 * uu / rr
    alpha1 = uu / (SHIFT * uu + (m * (m * dw - 2.0 * ww) + wz) - tilt * uu)
    e = alpha0 * (m + tilt)
    both_alpha = alpha0 * alpha1
    sol_d = alpha0 + alpha1 * e
    res_d = alpha0 * m - SHIFT * alpha1 * e
    res_w = -(alpha0 + alpha1 * e - SHIFT * both_alpha) - both_alpha
    res_z = both_alpha * NORM

    far_hop.wait_recv()
    give_hop.wait_recv()

    @pl.when(mine == 1)
    def _():
        give_rim.wait_recv()

    @pl.when(jnp.logical_and(mine == 0, me > 0))
    def _():
        next_even.wait_recv()

    @pl.when(jnp.logical_and(mine == 1, me > 0))
    def _():
        next_odd.wait_recv()

    def finish(l, dl, wl, zl):
        at = pl.ds(pl.multiple_of(l * width, width), width)
        out_ref[0, :, at] = sol_d * dl
        out_ref[1, :, at] = both_alpha * wl
        out_ref[2, :, at] = res_d * dl + res_w * wl
        out_ref[3, :, at] = res_z * zl

    for k in range(half):
        near = acc2[mine, k]
        far = part[k]
        if k < REACH:
            near = near + part[half + k]
            far = far + back[k]
        finish(base + k, probe_rows(mine, k), w[mine, k], near)
        finish(twin_base + k, own[:, k * width : (k + 1) * width], wfar[k], far)

    for copy in copies:
        copy.wait_send()
    for copy in (twin_hop, inner_hop, far_hop, give_hop):
        copy.wait_send()

    @pl.when(mine == 1)
    def _():
        ring_hop.wait_send()

    @pl.when(mine == 0)
    def _():
        give_rim.wait_send()

    @pl.when(jnp.logical_and(mine == 0, me > 0))
    def _():
        point_hop.wait_send()

    @pl.when(me > 0)
    def _():
        rim_hop.wait_send()

    @pl.when(has_edge)
    def _():
        for copy in edge_hops:
            copy.wait_send()

    @pl.when(jnp.logical_and(mine == 1, me < n - 1))
    def _():
        next_even.wait_send()
        next_odd.wait_send()


def body(coords, site_order, leaf_pairs, pair_count, probes):
    arrays = (coords, site_order, leaf_pairs, probes)
    n = lax.axis_size("leaf")
    leaf_dev, width = site_order.shape
    cols = probes.shape[0]
    half = leaf_dev // 2
    span = half + REACH
    slots_in = 2 * n - 1
    hbm = pl.BlockSpec(memory_space=pltpu.HBM)
    vmem = pl.BlockSpec(memory_space=pltpu.VMEM)
    field = functools.partial(pltpu.VMEM, dtype=F32)
    terms = pl.pallas_call(
        functools.partial(kernel, n),
        out_shape=jax.ShapeDtypeStruct((4, *probes.shape), F32),
        in_specs=[hbm] * 4,
        out_specs=vmem,
        scratch_shapes=[
            field(coords.shape),
            pltpu.VMEM(site_order.shape, jnp.int32),
            pltpu.VMEM(leaf_pairs.shape, jnp.int32),
            field((cols, half * width)),
            field((8, leaf_dev * width)),
            field((span, 8, width)),
            field((3, width, 128)),
            field((half * OFFS, 128)),
            pltpu.VMEM((half * OFFS, 2, width // 128, width, 128), BF16),
            field((2, cols, span * width)),
            field((2, span, cols, width)),
            field((half, cols, width)),
            pltpu.VMEM((span, 4 * cols, width), BF16),
            field((2, span, cols, width)),
            field((2, span, cols, width)),
            field((2, REACH, cols, width)),
            field((2, REACH, cols, width)),
            field((span, cols, width)),
            field((REACH, cols, width)),
            field((half, 2 * cols, width)),
            field((1, 128)),
            field((slots_in, 1, 128)),
            pltpu.SemaphoreType.REGULAR((2 * n.bit_length() + 2,)),
            pltpu.SemaphoreType.REGULAR,
            pltpu.SemaphoreType.DMA((6,)),
            pltpu.SemaphoreType.DMA((slots_in,)),
            pltpu.SemaphoreType.DMA((slots_in,)),
            pltpu.SemaphoreType.DMA((11,)),
            pltpu.SemaphoreType.DMA((11,)),
            pltpu.SemaphoreType.DMA((REACH,)),
            pltpu.SemaphoreType.DMA((REACH,)),
        ],
        compiler_params=pltpu.CompilerParams(
            collective_id=0, has_side_effects=True, vmem_limit_bytes=48 * 2**20
        ),
    )(*[pltpu.with_memory_space_constraint(x, pltpu.HBM) for x in arrays])

    return terms[0] - terms[1], terms[2] + terms[3]


def solution(mesh):
    in_specs = (P(None, "leaf"), P("leaf", None), P(None, "leaf"), P("leaf"), P("probe", "leaf"))
    out_specs = (P("probe", "leaf"), P("probe", "leaf"))
    return jax.shard_map(body, mesh=mesh, in_specs=in_specs, out_specs=out_specs, check_vma=False)
```

```python
import functools
import math

import jax
import jax.numpy as jnp
from jax import lax
from jax.experimental import pallas as pl
from jax.experimental.pallas import tpu as pltpu
from jax.sharding import PartitionSpec as P

REACH = 5
UNIT = 0.025
LENGTH = 0.12
NUGGET = 0.5
SHIFT = NUGGET + 1.0
TAPER = REACH * UNIT
GROW = math.sqrt(3.0) * TAPER / LENGTH
RATE = GROW / math.log(2.0)
QUAD = 4.0 * GROW
LIN = -(4.0 + 9.0 * GROW) * RATE / QUAD
CON = 5.0 * (1.0 + GROW) * RATE**2 / QUAD
NORM = QUAD * 2.0**-RATE / RATE**6
OFFS = REACH + 1
AHEAD = 1
ROWS = 32
MESH = pl.DeviceIdType.MESH
F32 = jnp.float32
BF16 = jnp.bfloat16


def dot(a, b, ca, cb):
    return lax.dot_general(a, b, (((ca,), (cb,)), ((), ())), preferred_element_type=F32)


def three(x, axis):
    hi = x.astype(BF16).astype(F32)
    mid = (x - hi).astype(BF16).astype(F32)
    return jnp.concatenate([hi, mid, x - hi - mid], axis=axis).astype(BF16)


def kernel(
    n, coords_hbm, order_hbm, pairs_hbm, probes_hbm, out_ref,
    cin, order, pairs, own, c8, prow, pcb, mask, tiles, d, w, wfar, v2, acc, acc2,
    in_edge, in_twin, part, back, diag, sum_out, sum_in, word, line_done, isem, ssem, rsem, hsend, hrecv, esend, erecv,
):
    leaf_dev, width = order.shape
    cols = probes_hbm.shape[0]
    half = leaf_dev // 2
    span = half + REACH
    me = lax.axis_index("leaf")
    probe = lax.axis_index("probe")
    mine = lax.rem(probe, 2)
    other = 1 - mine
    even = probe - mine
    twin = even + other
    base = half * mine
    twin_base = half * other
    after = lax.rem(me + 1, n)
    before = lax.rem(me + n - 1, n)
    edge_leaf = jnp.where(mine == 0, before, after)
    has_edge = jnp.where(mine == 0, me > 0, me < n - 1)
    edge = half * mine
    inner = half * other

    peers = [(k - 1, lax.rem(me + k, n), probe) for k in range(1, n)]
    peers += [(n - 1 + k, lax.rem(me + k, n), twin) for k in range(n)]
    slots_in = len(peers)

    def load(src, dst, slot):
        return pltpu.make_async_copy(src, dst, isem.at[slot])

    loads = [
        load(coords_hbm, cin, 0), load(order_hbm, order, 1), load(pairs_hbm, pairs, 2),
    ]
    def leaves(ref, first, count):
        return ref.at[:, pl.ds(pl.multiple_of(first * width, width), count * width)]

    def into_d(r, first, count):
        return d.at[r, :, first * width : (first + count) * width]

    loads.append(load(leaves(probes_hbm, base, half), into_d(mine, 0, half), 3))
    loads.append(load(leaves(probes_hbm, twin_base, half), own, 4))
    ring_load = load(leaves(probes_hbm, half, REACH), into_d(0, half, REACH), 5)
    for copy in loads:
        copy.start()

    @pl.when(mine == 0)
    def _():
        ring_load.start()

    barrier = pltpu.get_barrier_semaphore()
    def greet(sem, leaf, row):
        pl.semaphore_signal(
            sem, inc=1, device_id={"leaf": leaf, "probe": row}, device_id_type=MESH
        )

    greet(barrier, me, twin)

    @pl.when(me < n - 1)
    def _():
        greet(barrier, me + 1, probe)
        greet(barrier, me + 1, twin)

    steps = [1]
    while (1 << len(steps) - 1) < n - 1:
        steps.append(1 << len(steps) - 1)

    def tell(j):
        @pl.when(me >= steps[j])
        def _():
            greet(word.at[2 * j], me - steps[j], probe)

        if j > 0:

            @pl.when(me + steps[j] < n)
            def _():
                greet(word.at[2 * j + 1], me + steps[j], probe)

    def hear(j):
        @pl.when(me + steps[j] < n)
        def _():
            pl.semaphore_wait(word.at[2 * j], 1)

        if j > 0:

            @pl.when(me >= steps[j])
            def _():
                pl.semaphore_wait(word.at[2 * j + 1], 1)

    def hop(src, dst, slot, leaf, row, landing=None):
        return pltpu.make_async_remote_copy(
            src_ref=src, dst_ref=dst, send_sem=hsend.at[slot],
            recv_sem=hrecv.at[slot if landing is None else landing],
            device_id={"leaf": leaf, "probe": row}, device_id_type=MESH,
        )

    pl.semaphore_wait(barrier, 1 + jnp.where(me > 0, 2, 0))
    tell(0)

    point_hop = hop(prow.at[pl.ds(0, REACH)], prow.at[pl.ds(half, REACH)], 0, before, twin)
    rim_hop = hop(leaves(probes_hbm, 0, REACH), into_d(mine, half, REACH), 1, before, even + 1, 1 + mine)
    rim_in = [
        hop(leaves(probes_hbm, 0, REACH), into_d(k, half, REACH), 1, before, even + 1, 1 + k)
        for k in range(2)
    ]
    twin_hop = hop(leaves(probes_hbm, twin_base, half), into_d(mine, 0, half), 3, me, twin)
    ring_hop = hop(leaves(probes_hbm, half, REACH), into_d(mine, half, REACH), 4, me, twin)
    twin_hop.start()

    @pl.when(mine == 1)
    def _():
        ring_hop.start()

    @pl.when(me > 0)
    def _():
        rim_hop.start()

    place = lax.broadcasted_iota(jnp.int32, (width, width), 0)
    for copy in loads[:3]:
        copy.wait()
    c8[...] = jnp.zeros_like(c8)
    c8[0:3, :] = cin[...] * (RATE / TAPER)

    def gather(k):
        x = c8[:, pl.ds(pl.multiple_of((base + k) * width, width), width)]
        parts = three(x, 0)
        onehot = jnp.where(place == order[pl.ds(base + k, 1), :], 1.0, 0.0).astype(BF16)
        got = dot(parts, onehot, 1, 0)
        prow[k] = got[0:8] + got[8:16] + got[16:24]

    for k in range(half):
        gather(k)

    @pl.when(mine == 0)
    def _():
        for k in range(half, span):
            gather(k)

    slots = pairs.shape[1]
    first = pairs[0:1, :]
    second = pairs[1:2, :]
    code = (first - me * leaf_dev - base) * OFFS + (second - first)
    want = lax.broadcasted_iota(jnp.int32, (half * OFFS, slots), 0)
    hit = jnp.max(jnp.where(want == code, RATE, 0.0), axis=1, keepdims=True)
    mask[...] = jnp.broadcast_to(hit, mask.shape)
    acc[...] = jnp.zeros_like(acc)
    acc2[...] = jnp.zeros_like(acc2)

    @pl.when(jnp.logical_and(mine == 0, me > 0))
    def _():
        point_hop.start()

    def both(field, k):
        return jnp.concatenate([field[0, k], field[1, k]], axis=0)

    def probe_rows(r, k):
        return d[r, :, pl.ds(pl.multiple_of(k * width, width), width)]

    def both_probes(k):
        return jnp.concatenate([probe_rows(0, k), probe_rows(1, k)], axis=0)

    def stack(k, x):
        hi = x.astype(BF16)
        v2[k] = jnp.concatenate([hi, (x - hi.astype(F32)).astype(BF16)], axis=0)

    def add(into, k, x):
        into[0, k] += x[:cols]
        into[1, k] += x[cols:]

    rows = 2 * cols

    def tile(s):
        return [
            jnp.concatenate([tiles[s, p, h] for h in range(width // 128)], axis=1)
            for p in range(2)
        ]

    def columns(vi, hi, lo):
        x = dot(vi, hi, 1, 0)
        return x[:rows] + x[rows:] + dot(vi[:rows], lo, 1, 0)

    def products(i, into, make):
        vi = v2[i]
        row = jnp.zeros((2 * rows, width), F32)
        low = jnp.zeros((rows, width), F32)
        for o in [*range(1, OFFS), 0]:
            make(i, o)
            hi, lo = tile(i * OFFS + o)
            vj = v2[i + o]
            if o > 0:
                add(into, i + o, columns(vi, hi, lo))
                row = row + dot(vj, hi, 1, 1)
                low = low + dot(vj[:rows], lo, 1, 1)
            else:
                row = row + dot(vj, hi, 1, 0)
                low = low + dot(vj[:rows], lo, 1, 0)
        add(into, i, row[:rows] + row[rows:] + low)

    def first_products(i):
        vi = v2[i]
        for o in range(OFFS):
            hi, lo = tile(i * OFFS + o)
            x = columns(vi, hi, lo)
            if o > 0:
                add(acc2, i + o, x)
            else:
                diag[i] = x

    def last_products(i):
        row = jnp.zeros((2 * rows, width), F32)
        low = jnp.zeros((rows, width), F32)
        for o in range(1, OFFS):
            hi, lo = tile(i * OFFS + o)
            vj = v2[i + o]
            row = row + dot(vj, hi, 1, 1)
            low = low + dot(vj[:rows], lo, 1, 1)
        add(acc2, i, row[:rows] + row[rows:] + low + diag[i])

    def turn(i):
        turned = prow[i].T
        for c in range(3):
            pcb[c] = jnp.broadcast_to(turned[:, c : c + 1], (width, 128))

    def build(i, o):
        s = i * OFFS + o
        for h in range(width // 128):
            at = slice(h * 128, h * 128 + 128)
            listed = mask[pl.ds(s, 1), :]
            right = [
                jnp.broadcast_to(
                    jnp.where(listed > 0.0, prow[i + o, c : c + 1, at], prow[i, c : c + 1, at]),
                    (ROWS, 128),
                )
                for c in range(3)
            ]
            top = jnp.broadcast_to(listed, (ROWS, 128))
            for a in range(0, width if o > 0 else at.stop, ROWS):
                dx = pcb[0, a : a + ROWS, :] - right[0]
                dy = pcb[1, a : a + ROWS, :] - right[1]
                dz = pcb[2, a : a + ROWS, :] - right[2]
                d2 = jnp.maximum(dx * dx + dy * dy + dz * dz, 1e-30)
                y = jnp.maximum(top - d2 * lax.rsqrt(d2), 0.0)
                y2 = y * y
                t = (y2 * y2) * (y2 + (LIN * y + CON)) * jnp.exp2(y)
                hi = t.astype(BF16)
                tiles[s, 0, h, a : a + ROWS, :] = hi
                tiles[s, 1, h, a : a + ROWS, :] = (t - hi.astype(F32)).astype(BF16)
            if o == 0:
                for p in range(2):
                    for g in range(h):
                        block = tiles[s, p, h, g * 128 : g * 128 + 128, :]
                        tiles[s, p, g, h * 128 : h * 128 + 128, :] = block.T

    for copy in loads[3:]:
        copy.wait()

    @pl.when(mine == 0)
    def _():
        ring_load.wait()

    @pl.when(jnp.logical_and(mine == 1, me == n - 1))
    def _():
        d[:, :, half * width :] = jnp.zeros((2, cols, REACH * width), F32)
        prow[pl.ds(half, REACH)] = jnp.zeros((REACH, 8, width), F32)

    twin_hop.wait_recv()
    for k in range(half):
        stack(k, both_probes(k))

    edge_hops = []
    for j in range(REACH):
        seat = jnp.where(mine == 0, j, REACH - 1 - j)
        edge_hops.append(
            pltpu.make_async_remote_copy(
                src_ref=acc.at[:, edge + seat], dst_ref=in_edge.at[:, seat],
                send_sem=esend.at[seat], recv_sem=erecv.at[seat],
                device_id={"leaf": edge_leaf, "probe": twin}, device_id_type=MESH,
            )
        )
    inner_hop = hop(acc.at[:, pl.ds(inner, REACH)], in_twin, 6, me, twin)
    lag = half - REACH

    def leaf_at(t):
        late = jnp.where(t < AHEAD + REACH, half - 1 + AHEAD - t, t - REACH)
        return jnp.where(mine == 0, t, jnp.where(t < AHEAD, t, late))

    turn(0)

    def first_pass(t, carry):
        i = leaf_at(t)

        @pl.when(t == jnp.where(mine == 0, lag, AHEAD))
        def _():
            @pl.when(mine == 0)
            def _():
                ring_hop.wait_recv()

            @pl.when(jnp.logical_and(mine == 1, me < n - 1))
            def _():
                point_hop.wait_recv()
                for k in range(2):
                    rim_in[k].wait_recv()

            for k in range(half, span):
                stack(k, both_probes(k))

        for j in range(len(steps) - 1):
            @pl.when(t == j + 2)
            def _(j=j):
                hear(j)
                tell(j + 1)

        products(i, acc, build)
        turn(leaf_at(jnp.minimum(t + 1, half - 1)))

        for j in range(REACH):

            @pl.when(jnp.logical_and(t == j + AHEAD * mine, has_edge))
            def _(j=j):
                edge_hops[j].start()

        return carry

    lax.fori_loop(0, half, first_pass, 0)
    inner_hop.start()
    for j in range(half - 2, len(steps) - 1):
        hear(j)
        tell(j + 1)

    @pl.when(jnp.logical_not(has_edge))
    def _():
        in_edge[...] = jnp.zeros_like(in_edge)

    def make_w(k, more):
        xs = []
        for r in range(2):
            x = acc[r, k]
            if more is not None:
                x = x + more[r]
            x = NORM * x - probe_rows(r, k)
            w[r, k] = x
            xs.append(x)
        stack(k, jnp.concatenate(xs, axis=0))

    for k in range(REACH, half):
        make_w(k, None)

    @pl.when(has_edge)
    def _():
        for copy in edge_hops:
            copy.wait_recv()

    for k in range(REACH):
        make_w(edge + k, [in_edge[r, k] for r in range(2)])

    def outer_columns(t, carry):
        first_products(t + REACH * mine)
        return carry

    lax.fori_loop(0, lag, outer_columns, 0)
    inner_hop.wait_recv()
    for k in range(REACH):
        make_w(inner + k, [in_twin[r, k] for r in range(2)])

    far_hop = hop(w.at[other, pl.ds(0, half)], wfar, 7, me, twin)
    far_hop.start()
    give_hop = hop(acc2.at[other, pl.ds(0, half)], part.at[pl.ds(0, half)], 8, me, twin)
    give_rim = hop(acc2.at[other, pl.ds(half, REACH)], part.at[pl.ds(half, REACH)], 9, me, twin)
    next_even = hop(acc2.at[0, pl.ds(half, REACH)], part.at[pl.ds(half, REACH)], 9, after, even)
    next_odd = hop(acc2.at[1, pl.ds(half, REACH)], back, 10, after, even + 1)

    left = lag * other

    def first_half(t, carry):
        i = left + REACH - 1 - t
        first_products(i)

        @pl.when(jnp.logical_and(i == lag, mine == 0))
        def _():
            give_rim.start()

        @pl.when(jnp.logical_and(i == lag, jnp.logical_and(mine == 1, me < n - 1)))
        def _():
            next_even.start()
            next_odd.start()

        return carry

    hear(len(steps) - 1)
    greet(line_done, me, twin)
    lax.fori_loop(0, REACH, first_half, 0)

    def lanes(x):
        return x[:, :128] + x[:, 128:] if width == 256 else x

    sums = [jnp.zeros((rows, width), F32) for _ in range(4)]
    own_part = jnp.zeros((rows, width), F32)
    for k in range(span):
        wk = both(w, k)
        sums[3] = sums[3] + wk * both(acc2, k)
        if k < half:
            own_part = own_part + wk * diag[k]
        if k < half:
            dk = both_probes(k)
            sums[0] = sums[0] + dk * dk
            sums[1] = sums[1] + dk * wk
            sums[2] = sums[2] + wk * wk
    sums[3] = 2.0 * sums[3] + own_part
    stacked = jnp.concatenate([lanes(x) for x in sums], axis=0)
    parts = three(stacked, 1)
    total = dot(jnp.full((8, parts.shape[1]), 1.0, BF16), parts, 1, 1)
    sum_out[...] = total[0:1]
    pl.semaphore_wait(line_done, 1)
    copies = []
    for slot, leaf, row in peers:
        copy = pltpu.make_async_remote_copy(
            src_ref=sum_out, dst_ref=sum_in.at[slot],
            send_sem=ssem.at[slot], recv_sem=rsem.at[slot],
            device_id={"leaf": leaf, "probe": row}, device_id_type=MESH,
        )
        copy.start()
        copies.append(copy)

    def last_half(i, carry):
        last_products(i)
        return carry

    lax.fori_loop(0, half, last_half, 0)
    give_hop.start()

    @pl.when(jnp.logical_and(mine == 0, me == 0))
    def _():
        part[pl.ds(half, REACH)] = jnp.zeros((REACH, cols, width), F32)

    @pl.when(jnp.logical_and(mine == 1, me == 0))
    def _():
        back[...] = jnp.zeros_like(back)

    @pl.when(mine == 0)
    def _():
        back[...] = acc2[0, pl.ds(half, REACH)]

    total = sum_out[...]
    for slot, copy in enumerate(copies):
        copy.wait_recv()
        total = total + sum_in[slot]
    column = lax.broadcasted_iota(jnp.int32, (cols, 128), 1)
    line = lax.broadcasted_iota(jnp.int32, (cols, 128), 0) + mine * cols
    rr, dw, ww, wk = [
        jnp.sum(jnp.where(column == line + q * rows, total, 0.0), axis=1, keepdims=True)
        for q in range(4)
    ]
    wz = NORM * wk - ww
    m = dw / rr
    alpha0 = rr / (SHIFT * rr + dw)
    uu = ww - m * dw
    tilt = alpha0 * uu / rr
    alpha1 = uu / (SHIFT * uu + (m * (m * dw - 2.0 * ww) + wz) - tilt * uu)
    e = alpha0 * (m + tilt)
    both_alpha = alpha0 * alpha1
    sol_d = alpha0 + alpha1 * e
    res_d = alpha0 * m - SHIFT * alpha1 * e
    res_w = -(alpha0 + alpha1 * e - SHIFT * both_alpha) - both_alpha
    res_z = both_alpha * NORM

    far_hop.wait_recv()
    give_hop.wait_recv()

    @pl.when(mine == 1)
    def _():
        give_rim.wait_recv()

    @pl.when(jnp.logical_and(mine == 0, me > 0))
    def _():
        next_even.wait_recv()

    @pl.when(jnp.logical_and(mine == 1, me > 0))
    def _():
        next_odd.wait_recv()

    def finish(l, dl, wl, zl):
        at = pl.ds(pl.multiple_of(l * width, width), width)
        out_ref[0, :, at] = sol_d * dl
        out_ref[1, :, at] = both_alpha * wl
        out_ref[2, :, at] = res_d * dl + res_w * wl
        out_ref[3, :, at] = res_z * zl

    for k in range(half):
        near = acc2[mine, k]
        far = part[k]
        if k < REACH:
            near = near + part[half + k]
            far = far + back[k]
        finish(base + k, probe_rows(mine, k), w[mine, k], near)
        finish(twin_base + k, own[:, k * width : (k + 1) * width], wfar[k], far)

    for copy in copies:
        copy.wait_send()
    for copy in (twin_hop, inner_hop, far_hop, give_hop):
        copy.wait_send()

    @pl.when(mine == 1)
    def _():
        ring_hop.wait_send()

    @pl.when(mine == 0)
    def _():
        give_rim.wait_send()

    @pl.when(jnp.logical_and(mine == 0, me > 0))
    def _():
        point_hop.wait_send()

    @pl.when(me > 0)
    def _():
        rim_hop.wait_send()

    @pl.when(has_edge)
    def _():
        for copy in edge_hops:
            copy.wait_send()

    @pl.when(jnp.logical_and(mine == 1, me < n - 1))
    def _():
        next_even.wait_send()
        next_odd.wait_send()


def body(coords, site_order, leaf_pairs, pair_count, probes):
    arrays = (coords, site_order, leaf_pairs, probes)
    n = lax.axis_size("leaf")
    leaf_dev, width = site_order.shape
    cols = probes.shape[0]
    half = leaf_dev // 2
    span = half + REACH
    slots_in = 2 * n - 1
    hbm = pl.BlockSpec(memory_space=pltpu.HBM)
    vmem = pl.BlockSpec(memory_space=pltpu.VMEM)
    field = functools.partial(pltpu.VMEM, dtype=F32)
    terms = pl.pallas_call(
        functools.partial(kernel, n),
        out_shape=jax.ShapeDtypeStruct((4, *probes.shape), F32),
        in_specs=[hbm] * 4,
        out_specs=vmem,
        scratch_shapes=[
            field(coords.shape),
            pltpu.VMEM(site_order.shape, jnp.int32),
            pltpu.VMEM(leaf_pairs.shape, jnp.int32),
            field((cols, half * width)),
            field((8, leaf_dev * width)),
            field((span, 8, width)),
            field((3, width, 128)),
            field((half * OFFS, 128)),
            pltpu.VMEM((half * OFFS, 2, width // 128, width, 128), BF16),
            field((2, cols, span * width)),
            field((2, span, cols, width)),
            field((half, cols, width)),
            pltpu.VMEM((span, 4 * cols, width), BF16),
            field((2, span, cols, width)),
            field((2, span, cols, width)),
            field((2, REACH, cols, width)),
            field((2, REACH, cols, width)),
            field((span, cols, width)),
            field((REACH, cols, width)),
            field((half, 2 * cols, width)),
            field((1, 128)),
            field((slots_in, 1, 128)),
            pltpu.SemaphoreType.REGULAR((2 * n.bit_length() + 2,)),
            pltpu.SemaphoreType.REGULAR,
            pltpu.SemaphoreType.DMA((6,)),
            pltpu.SemaphoreType.DMA((slots_in,)),
            pltpu.SemaphoreType.DMA((slots_in,)),
            pltpu.SemaphoreType.DMA((11,)),
            pltpu.SemaphoreType.DMA((11,)),
            pltpu.SemaphoreType.DMA((REACH,)),
            pltpu.SemaphoreType.DMA((REACH,)),
        ],
        compiler_params=pltpu.CompilerParams(
            collective_id=0, has_side_effects=True, vmem_limit_bytes=48 * 2**20
        ),
    )(*[pltpu.with_memory_space_constraint(x, pltpu.HBM) for x in arrays])

    return terms[0] - terms[1], terms[2] + terms[3]


def solution(mesh):
    in_specs = (P(None, "leaf"), P("leaf", None), P(None, "leaf"), P("leaf"), P("probe", "leaf"))
    out_specs = (P("probe", "leaf"), P("probe", "leaf"))
    return jax.shard_map(body, mesh=mesh, in_specs=in_specs, out_specs=out_specs, check_vma=False)
```

```python
import functools
import math

import jax
import jax.numpy as jnp
from jax import lax
from jax.experimental import pallas as pl
from jax.experimental.pallas import tpu as pltpu
from jax.sharding import PartitionSpec as P

REACH = 5
UNIT = 0.025
LENGTH = 0.12
NUGGET = 0.5
SHIFT = NUGGET + 1.0
TAPER = REACH * UNIT
GROW = math.sqrt(3.0) * TAPER / LENGTH
RATE = GROW / math.log(2.0)
QUAD = 4.0 * GROW
LIN = -(4.0 + 9.0 * GROW) * RATE / QUAD
CON = 5.0 * (1.0 + GROW) * RATE**2 / QUAD
NORM = QUAD * 2.0**-RATE / RATE**6
OFFS = REACH + 1
AHEAD = 1
ROWS = 32
MESH = pl.DeviceIdType.MESH
F32 = jnp.float32
BF16 = jnp.bfloat16


def dot(a, b, ca, cb):
    return lax.dot_general(a, b, (((ca,), (cb,)), ((), ())), preferred_element_type=F32)


def three(x, axis):
    hi = x.astype(BF16).astype(F32)
    mid = (x - hi).astype(BF16).astype(F32)
    return jnp.concatenate([hi, mid, x - hi - mid], axis=axis).astype(BF16)


def kernel(
    n, coords_hbm, order_hbm, pairs_hbm, probes_hbm, out_ref,
    cin, order, pairs, own, c8, prow, pcb, mask, tiles, d, w, wfar, v2, acc, acc2,
    in_edge, in_twin, part, back, diag, sum_out, sum_in, word, line_done, isem, ssem, rsem, hsend, hrecv, esend, erecv,
):
    leaf_dev, width = order.shape
    cols = probes_hbm.shape[0]
    half = leaf_dev // 2
    span = half + REACH
    me = lax.axis_index("leaf")
    probe = lax.axis_index("probe")
    mine = lax.rem(probe, 2)
    other = 1 - mine
    even = probe - mine
    twin = even + other
    base = half * mine
    twin_base = half * other
    after = lax.rem(me + 1, n)
    before = lax.rem(me + n - 1, n)
    edge_leaf = jnp.where(mine == 0, before, after)
    has_edge = jnp.where(mine == 0, me > 0, me < n - 1)
    edge = half * mine
    inner = half * other

    peers = [(k - 1, lax.rem(me + k, n), probe) for k in range(1, n)]
    peers += [(n - 1 + k, lax.rem(me + k, n), twin) for k in range(n)]
    slots_in = len(peers)

    def load(src, dst, slot):
        return pltpu.make_async_copy(src, dst, isem.at[slot])

    loads = [
        load(coords_hbm, cin, 0), load(order_hbm, order, 1), load(pairs_hbm, pairs, 2),
    ]
    def leaves(ref, first, count):
        return ref.at[:, pl.ds(pl.multiple_of(first * width, width), count * width)]

    def into_d(r, first, count):
        return d.at[r, :, first * width : (first + count) * width]

    loads.append(load(leaves(probes_hbm, base, half), into_d(mine, 0, half), 3))
    loads.append(load(leaves(probes_hbm, twin_base, half), own, 4))
    ring_load = load(leaves(probes_hbm, half, REACH), into_d(0, half, REACH), 5)
    for copy in loads:
        copy.start()

    @pl.when(mine == 0)
    def _():
        ring_load.start()

    barrier = pltpu.get_barrier_semaphore()
    def greet(sem, leaf, row):
        pl.semaphore_signal(
            sem, inc=1, device_id={"leaf": leaf, "probe": row}, device_id_type=MESH
        )

    greet(barrier, me, twin)

    @pl.when(me < n - 1)
    def _():
        greet(barrier, me + 1, probe)
        greet(barrier, me + 1, twin)

    steps = [1]
    while (1 << len(steps) - 1) < n - 1:
        steps.append(1 << len(steps) - 1)

    def tell(j):
        @pl.when(me >= steps[j])
        def _():
            greet(word.at[2 * j], me - steps[j], probe)

        if j > 0:

            @pl.when(me + steps[j] < n)
            def _():
                greet(word.at[2 * j + 1], me + steps[j], probe)

    def hear(j):
        @pl.when(me + steps[j] < n)
        def _():
            pl.semaphore_wait(word.at[2 * j], 1)

        if j > 0:

            @pl.when(me >= steps[j])
            def _():
                pl.semaphore_wait(word.at[2 * j + 1], 1)

    def hop(src, dst, slot, leaf, row, landing=None):
        return pltpu.make_async_remote_copy(
            src_ref=src, dst_ref=dst, send_sem=hsend.at[slot],
            recv_sem=hrecv.at[slot if landing is None else landing],
            device_id={"leaf": leaf, "probe": row}, device_id_type=MESH,
        )

    pl.semaphore_wait(barrier, 1 + jnp.where(me > 0, 2, 0))
    tell(0)

    point_hop = hop(prow.at[pl.ds(0, REACH)], prow.at[pl.ds(half, REACH)], 0, before, twin)
    rim_hop = hop(leaves(probes_hbm, 0, REACH), into_d(mine, half, REACH), 1, before, even + 1, 1 + mine)
    rim_in = [
        hop(leaves(probes_hbm, 0, REACH), into_d(k, half, REACH), 1, before, even + 1, 1 + k)
        for k in range(2)
    ]
    twin_hop = hop(leaves(probes_hbm, twin_base, half), into_d(mine, 0, half), 3, me, twin)
    ring_hop = hop(leaves(probes_hbm, half, REACH), into_d(mine, half, REACH), 4, me, twin)
    twin_hop.start()

    @pl.when(mine == 1)
    def _():
        ring_hop.start()

    @pl.when(me > 0)
    def _():
        rim_hop.start()

    place = lax.broadcasted_iota(jnp.int32, (width, width), 0)
    for copy in loads[:3]:
        copy.wait()
    c8[...] = jnp.zeros_like(c8)
    c8[0:3, :] = cin[...] * (RATE / TAPER)

    def gather(k):
        x = c8[:, pl.ds(pl.multiple_of((base + k) * width, width), width)]
        parts = three(x, 0)
        onehot = jnp.where(place == order[pl.ds(base + k, 1), :], 1.0, 0.0).astype(BF16)
        got = dot(parts, onehot, 1, 0)
        prow[k] = got[0:8] + got[8:16] + got[16:24]

    for k in range(half):
        gather(k)

    @pl.when(mine == 0)
    def _():
        for k in range(half, span):
            gather(k)

    slots = pairs.shape[1]
    first = pairs[0:1, :]
    second = pairs[1:2, :]
    code = (first - me * leaf_dev - base) * OFFS + (second - first)
    want = lax.broadcasted_iota(jnp.int32, (half * OFFS, slots), 0)
    hit = jnp.max(jnp.where(want == code, RATE, 0.0), axis=1, keepdims=True)
    mask[...] = jnp.broadcast_to(hit, mask.shape)
    acc[...] = jnp.zeros_like(acc)
    acc2[...] = jnp.zeros_like(acc2)

    @pl.when(jnp.logical_and(mine == 0, me > 0))
    def _():
        point_hop.start()

    def both(field, k):
        return jnp.concatenate([field[0, k], field[1, k]], axis=0)

    def probe_rows(r, k):
        return d[r, :, pl.ds(pl.multiple_of(k * width, width), width)]

    def both_probes(k):
        return jnp.concatenate([probe_rows(0, k), probe_rows(1, k)], axis=0)

    def stack(k, x):
        hi = x.astype(BF16)
        v2[k] = jnp.concatenate([hi, (x - hi.astype(F32)).astype(BF16)], axis=0)

    def add(into, k, x):
        into[0, k] += x[:cols]
        into[1, k] += x[cols:]

    rows = 2 * cols

    def tile(s):
        return [
            jnp.concatenate([tiles[s, p, h] for h in range(width // 128)], axis=1)
            for p in range(2)
        ]

    def columns(vi, hi, lo):
        x = dot(vi, hi, 1, 0)
        return x[:rows] + x[rows:] + dot(vi[:rows], lo, 1, 0)

    def products(i, into, make):
        vi = v2[i]
        row = jnp.zeros((2 * rows, width), F32)
        low = jnp.zeros((rows, width), F32)
        for o in [*range(1, OFFS), 0]:
            make(i, o)
            hi, lo = tile(i * OFFS + o)
            vj = v2[i + o]
            if o > 0:
                add(into, i + o, columns(vi, hi, lo))
                row = row + dot(vj, hi, 1, 1)
                low = low + dot(vj[:rows], lo, 1, 1)
            else:
                row = row + dot(vj, hi, 1, 0)
                low = low + dot(vj[:rows], lo, 1, 0)
        add(into, i, row[:rows] + row[rows:] + low)

    def first_products(i):
        vi = v2[i]
        for o in range(OFFS):
            hi, lo = tile(i * OFFS + o)
            x = columns(vi, hi, lo)
            if o > 0:
                add(acc2, i + o, x)
            else:
                diag[i] = x

    def last_products(i):
        row = jnp.zeros((2 * rows, width), F32)
        low = jnp.zeros((rows, width), F32)
        for o in range(1, OFFS):
            hi, lo = tile(i * OFFS + o)
            vj = v2[i + o]
            row = row + dot(vj, hi, 1, 1)
            low = low + dot(vj[:rows], lo, 1, 1)
        add(acc2, i, row[:rows] + row[rows:] + low + diag[i])

    def turn(i):
        turned = prow[i].T
        for c in range(3):
            pcb[c] = jnp.broadcast_to(turned[:, c : c + 1], (width, 128))

    def build(i, o):
        s = i * OFFS + o
        for h in range(width // 128):
            at = slice(h * 128, h * 128 + 128)
            listed = mask[pl.ds(s, 1), :]
            right = [
                jnp.broadcast_to(
                    jnp.where(listed > 0.0, prow[i + o, c : c + 1, at], prow[i, c : c + 1, at]),
                    (ROWS, 128),
                )
                for c in range(3)
            ]
            top = jnp.broadcast_to(listed, (ROWS, 128))
            for a in range(0, width if o > 0 else at.stop, ROWS):
                dx = pcb[0, a : a + ROWS, :] - right[0]
                dy = pcb[1, a : a + ROWS, :] - right[1]
                dz = pcb[2, a : a + ROWS, :] - right[2]
                d2 = jnp.maximum(dx * dx + dy * dy + dz * dz, 1e-30)
                y = jnp.maximum(top - d2 * lax.rsqrt(d2), 0.0)
                y2 = y * y
                t = (y2 * y2) * (y2 + (LIN * y + CON)) * jnp.exp2(y)
                hi = t.astype(BF16)
                tiles[s, 0, h, a : a + ROWS, :] = hi
                tiles[s, 1, h, a : a + ROWS, :] = (t - hi.astype(F32)).astype(BF16)
            if o == 0:
                for p in range(2):
                    for g in range(h):
                        block = tiles[s, p, h, g * 128 : g * 128 + 128, :]
                        tiles[s, p, g, h * 128 : h * 128 + 128, :] = block.T

    for copy in loads[3:]:
        copy.wait()

    @pl.when(mine == 0)
    def _():
        ring_load.wait()

    @pl.when(jnp.logical_and(mine == 1, me == n - 1))
    def _():
        d[:, :, half * width :] = jnp.zeros((2, cols, REACH * width), F32)
        prow[pl.ds(half, REACH)] = jnp.zeros((REACH, 8, width), F32)

    twin_hop.wait_recv()
    for k in range(half):
        stack(k, both_probes(k))

    edge_hops = []
    for j in range(REACH):
        seat = jnp.where(mine == 0, j, REACH - 1 - j)
        edge_hops.append(
            pltpu.make_async_remote_copy(
                src_ref=acc.at[:, edge + seat], dst_ref=in_edge.at[:, seat],
                send_sem=esend.at[seat], recv_sem=erecv.at[seat],
                device_id={"leaf": edge_leaf, "probe": twin}, device_id_type=MESH,
            )
        )
    inner_hop = hop(acc.at[:, pl.ds(inner, REACH)], in_twin, 6, me, twin)
    lag = half - REACH

    def leaf_at(t):
        late = jnp.where(t < AHEAD + REACH, half - 1 + AHEAD - t, t - REACH)
        return jnp.where(mine == 0, t, jnp.where(t < AHEAD, t, late))

    turn(0)

    def first_pass(t, carry):
        i = leaf_at(t)

        @pl.when(t == jnp.where(mine == 0, lag, AHEAD))
        def _():
            @pl.when(mine == 0)
            def _():
                ring_hop.wait_recv()

            @pl.when(jnp.logical_and(mine == 1, me < n - 1))
            def _():
                point_hop.wait_recv()
                for k in range(2):
                    rim_in[k].wait_recv()

            for k in range(half, span):
                stack(k, both_probes(k))

        for j in range(len(steps) - 1):
            @pl.when(t == j + 2)
            def _(j=j):
                hear(j)
                tell(j + 1)

        products(i, acc, build)
        turn(leaf_at(jnp.minimum(t + 1, half - 1)))

        for j in range(REACH):

            @pl.when(jnp.logical_and(t == j + AHEAD * mine, has_edge))
            def _(j=j):
                edge_hops[j].start()

        return carry

    lax.fori_loop(0, half, first_pass, 0)
    inner_hop.start()
    for j in range(half - 2, len(steps) - 1):
        hear(j)
        tell(j + 1)

    @pl.when(jnp.logical_not(has_edge))
    def _():
        in_edge[...] = jnp.zeros_like(in_edge)

    def make_w(k, more):
        xs = []
        for r in range(2):
            x = acc[r, k]
            if more is not None:
                x = x + more[r]
            x = NORM * x - probe_rows(r, k)
            w[r, k] = x
            xs.append(x)
        stack(k, jnp.concatenate(xs, axis=0))

    for k in range(REACH, half):
        make_w(k, None)

    @pl.when(has_edge)
    def _():
        for copy in edge_hops:
            copy.wait_recv()

    for k in range(REACH):
        make_w(edge + k, [in_edge[r, k] for r in range(2)])

    def outer_columns(t, carry):
        first_products(t + REACH * mine)
        return carry

    lax.fori_loop(0, lag, outer_columns, 0, unroll=True)
    inner_hop.wait_recv()
    for k in range(REACH):
        make_w(inner + k, [in_twin[r, k] for r in range(2)])

    far_hop = hop(w.at[other, pl.ds(0, half)], wfar, 7, me, twin)
    far_hop.start()
    give_hop = hop(acc2.at[other, pl.ds(0, half)], part.at[pl.ds(0, half)], 8, me, twin)
    give_rim = hop(acc2.at[other, pl.ds(half, REACH)], part.at[pl.ds(half, REACH)], 9, me, twin)
    next_even = hop(acc2.at[0, pl.ds(half, REACH)], part.at[pl.ds(half, REACH)], 9, after, even)
    next_odd = hop(acc2.at[1, pl.ds(half, REACH)], back, 10, after, even + 1)

    left = lag * other

    hear(len(steps) - 1)
    greet(line_done, me, twin)
    for t in range(REACH):
        first_products(left + REACH - 1 - t)
        if t == 2 * REACH - half - 1:

            @pl.when(jnp.logical_and(mine == 1, me < n - 1))
            def _():
                next_even.start()
                next_odd.start()

    @pl.when(mine == 0)
    def _():
        give_rim.start()


    def lanes(x):
        return x[:, :128] + x[:, 128:] if width == 256 else x

    sums = [jnp.zeros((rows, width), F32) for _ in range(4)]
    own_part = jnp.zeros((rows, width), F32)
    for k in range(span):
        wk = both(w, k)
        sums[3] = sums[3] + wk * both(acc2, k)
        if k < half:
            own_part = own_part + wk * diag[k]
        if k < half:
            dk = both_probes(k)
            sums[0] = sums[0] + dk * dk
            sums[1] = sums[1] + dk * wk
            sums[2] = sums[2] + wk * wk
    sums[3] = 2.0 * sums[3] + own_part
    stacked = jnp.concatenate([lanes(x) for x in sums], axis=0)
    parts = three(stacked, 1)
    total = dot(jnp.full((8, parts.shape[1]), 1.0, BF16), parts, 1, 1)
    sum_out[...] = total[0:1]
    pl.semaphore_wait(line_done, 1)
    copies = []
    for slot, leaf, row in peers:
        copy = pltpu.make_async_remote_copy(
            src_ref=sum_out, dst_ref=sum_in.at[slot],
            send_sem=ssem.at[slot], recv_sem=rsem.at[slot],
            device_id={"leaf": leaf, "probe": row}, device_id_type=MESH,
        )
        copy.start()
        copies.append(copy)

    def last_half(i, carry):
        last_products(i)
        return carry

    lax.fori_loop(0, half, last_half, 0, unroll=2)
    give_hop.start()

    @pl.when(jnp.logical_and(mine == 0, me == 0))
    def _():
        part[pl.ds(half, REACH)] = jnp.zeros((REACH, cols, width), F32)

    @pl.when(jnp.logical_and(mine == 1, me == 0))
    def _():
        back[...] = jnp.zeros_like(back)

    @pl.when(mine == 0)
    def _():
        back[...] = acc2[0, pl.ds(half, REACH)]

    total = sum_out[...]
    for slot, copy in enumerate(copies):
        copy.wait_recv()
        total = total + sum_in[slot]
    column = lax.broadcasted_iota(jnp.int32, (cols, 128), 1)
    line = lax.broadcasted_iota(jnp.int32, (cols, 128), 0) + mine * cols
    rr, dw, ww, wk = [
        jnp.sum(jnp.where(column == line + q * rows, total, 0.0), axis=1, keepdims=True)
        for q in range(4)
    ]
    wz = NORM * wk - ww
    m = dw / rr
    alpha0 = rr / (SHIFT * rr + dw)
    uu = ww - m * dw
    tilt = alpha0 * uu / rr
    alpha1 = uu / (SHIFT * uu + (m * (m * dw - 2.0 * ww) + wz) - tilt * uu)
    e = alpha0 * (m + tilt)
    both_alpha = alpha0 * alpha1
    sol_d = alpha0 + alpha1 * e
    res_d = alpha0 * m - SHIFT * alpha1 * e
    res_w = -(alpha0 + alpha1 * e - SHIFT * both_alpha) - both_alpha
    res_z = both_alpha * NORM

    far_hop.wait_recv()
    give_hop.wait_recv()

    @pl.when(mine == 1)
    def _():
        give_rim.wait_recv()

    @pl.when(jnp.logical_and(mine == 0, me > 0))
    def _():
        next_even.wait_recv()

    @pl.when(jnp.logical_and(mine == 1, me > 0))
    def _():
        next_odd.wait_recv()

    def finish(l, dl, wl, zl):
        at = pl.ds(pl.multiple_of(l * width, width), width)
        out_ref[0, :, at] = sol_d * dl
        out_ref[1, :, at] = both_alpha * wl
        out_ref[2, :, at] = res_d * dl + res_w * wl
        out_ref[3, :, at] = res_z * zl

    for k in range(half):
        near = acc2[mine, k]
        far = part[k]
        if k < REACH:
            near = near + part[half + k]
            far = far + back[k]
        finish(base + k, probe_rows(mine, k), w[mine, k], near)
        finish(twin_base + k, own[:, k * width : (k + 1) * width], wfar[k], far)

    for copy in copies:
        copy.wait_send()
    for copy in (twin_hop, inner_hop, far_hop, give_hop):
        copy.wait_send()

    @pl.when(mine == 1)
    def _():
        ring_hop.wait_send()

    @pl.when(mine == 0)
    def _():
        give_rim.wait_send()

    @pl.when(jnp.logical_and(mine == 0, me > 0))
    def _():
        point_hop.wait_send()

    @pl.when(me > 0)
    def _():
        rim_hop.wait_send()

    @pl.when(has_edge)
    def _():
        for copy in edge_hops:
            copy.wait_send()

    @pl.when(jnp.logical_and(mine == 1, me < n - 1))
    def _():
        next_even.wait_send()
        next_odd.wait_send()


def body(coords, site_order, leaf_pairs, pair_count, probes):
    arrays = (coords, site_order, leaf_pairs, probes)
    n = lax.axis_size("leaf")
    leaf_dev, width = site_order.shape
    cols = probes.shape[0]
    half = leaf_dev // 2
    span = half + REACH
    slots_in = 2 * n - 1
    hbm = pl.BlockSpec(memory_space=pltpu.HBM)
    vmem = pl.BlockSpec(memory_space=pltpu.VMEM)
    field = functools.partial(pltpu.VMEM, dtype=F32)
    terms = pl.pallas_call(
        functools.partial(kernel, n),
        out_shape=jax.ShapeDtypeStruct((4, *probes.shape), F32),
        in_specs=[hbm] * 4,
        out_specs=vmem,
        scratch_shapes=[
            field(coords.shape),
            pltpu.VMEM(site_order.shape, jnp.int32),
            pltpu.VMEM(leaf_pairs.shape, jnp.int32),
            field((cols, half * width)),
            field((8, leaf_dev * width)),
            field((span, 8, width)),
            field((3, width, 128)),
            field((half * OFFS, 128)),
            pltpu.VMEM((half * OFFS, 2, width // 128, width, 128), BF16),
            field((2, cols, span * width)),
            field((2, span, cols, width)),
            field((half, cols, width)),
            pltpu.VMEM((span, 4 * cols, width), BF16),
            field((2, span, cols, width)),
            field((2, span, cols, width)),
            field((2, REACH, cols, width)),
            field((2, REACH, cols, width)),
            field((span, cols, width)),
            field((REACH, cols, width)),
            field((half, 2 * cols, width)),
            field((1, 128)),
            field((slots_in, 1, 128)),
            pltpu.SemaphoreType.REGULAR((2 * n.bit_length() + 2,)),
            pltpu.SemaphoreType.REGULAR,
            pltpu.SemaphoreType.DMA((6,)),
            pltpu.SemaphoreType.DMA((slots_in,)),
            pltpu.SemaphoreType.DMA((slots_in,)),
            pltpu.SemaphoreType.DMA((11,)),
            pltpu.SemaphoreType.DMA((11,)),
            pltpu.SemaphoreType.DMA((REACH,)),
            pltpu.SemaphoreType.DMA((REACH,)),
        ],
        compiler_params=pltpu.CompilerParams(
            collective_id=0, has_side_effects=True, vmem_limit_bytes=48 * 2**20
        ),
    )(*[pltpu.with_memory_space_constraint(x, pltpu.HBM) for x in arrays])

    return terms[0] - terms[1], terms[2] + terms[3]


def solution(mesh):
    in_specs = (P(None, "leaf"), P("leaf", None), P(None, "leaf"), P("leaf"), P("probe", "leaf"))
    out_specs = (P("probe", "leaf"), P("probe", "leaf"))
    return jax.shard_map(body, mesh=mesh, in_specs=in_specs, out_specs=out_specs, check_vma=False)
```

```python
import functools
import math

import jax
import jax.numpy as jnp
from jax import lax
from jax.experimental import pallas as pl
from jax.experimental.pallas import tpu as pltpu
from jax.sharding import PartitionSpec as P

REACH = 5
UNIT = 0.025
LENGTH = 0.12
NUGGET = 0.5
SHIFT = NUGGET + 1.0
TAPER = REACH * UNIT
GROW = math.sqrt(3.0) * TAPER / LENGTH
RATE = GROW / math.log(2.0)
QUAD = 4.0 * GROW
LIN = -(4.0 + 9.0 * GROW) * RATE / QUAD
CON = 5.0 * (1.0 + GROW) * RATE**2 / QUAD
NORM = QUAD * 2.0**-RATE / RATE**6
OFFS = REACH + 1
AHEAD = 1
ROWS = 32
MESH = pl.DeviceIdType.MESH
F32 = jnp.float32
BF16 = jnp.bfloat16


def dot(a, b, ca, cb):
    return lax.dot_general(a, b, (((ca,), (cb,)), ((), ())), preferred_element_type=F32)


def three(x, axis):
    hi = x.astype(BF16).astype(F32)
    mid = (x - hi).astype(BF16).astype(F32)
    return jnp.concatenate([hi, mid, x - hi - mid], axis=axis).astype(BF16)


def kernel(
    n, coords_hbm, order_hbm, pairs_hbm, probes_hbm, out_ref,
    cin, order, pairs, own, c8, prow, pcb, mask, tiles, d, w, wfar, v2, acc, acc2,
    in_edge, in_twin, part, back, diag, sum_out, sum_in, word, line_done, isem, ssem, rsem, hsend, hrecv, esend, erecv,
):
    leaf_dev, width = order.shape
    cols = probes_hbm.shape[0]
    half = leaf_dev // 2
    span = half + REACH
    me = lax.axis_index("leaf")
    probe = lax.axis_index("probe")
    mine = lax.rem(probe, 2)
    other = 1 - mine
    even = probe - mine
    twin = even + other
    base = half * mine
    twin_base = half * other
    after = lax.rem(me + 1, n)
    before = lax.rem(me + n - 1, n)
    edge_leaf = jnp.where(mine == 0, before, after)
    has_edge = jnp.where(mine == 0, me > 0, me < n - 1)
    edge = half * mine
    inner = half * other

    peers = [(k - 1, lax.rem(me + k, n), probe) for k in range(1, n)]
    peers += [(n - 1 + k, lax.rem(me + k, n), twin) for k in range(n)]
    slots_in = len(peers)

    def load(src, dst, slot):
        return pltpu.make_async_copy(src, dst, isem.at[slot])

    loads = [
        load(coords_hbm, cin, 0), load(order_hbm, order, 1), load(pairs_hbm, pairs, 2),
    ]
    def leaves(ref, first, count):
        return ref.at[:, pl.ds(pl.multiple_of(first * width, width), count * width)]

    def into_d(r, first, count):
        return d.at[r, :, first * width : (first + count) * width]

    loads.append(load(leaves(probes_hbm, base, half), into_d(mine, 0, half), 3))
    loads.append(load(leaves(probes_hbm, twin_base, half), own, 4))
    ring_load = load(leaves(probes_hbm, half, REACH), into_d(0, half, REACH), 5)
    for copy in loads:
        copy.start()

    @pl.when(mine == 0)
    def _():
        ring_load.start()

    barrier = pltpu.get_barrier_semaphore()
    def greet(sem, leaf, row):
        pl.semaphore_signal(
            sem, inc=1, device_id={"leaf": leaf, "probe": row}, device_id_type=MESH
        )

    greet(barrier, me, twin)

    @pl.when(me < n - 1)
    def _():
        greet(barrier, me + 1, probe)
        greet(barrier, me + 1, twin)

    steps = [1]
    while (1 << len(steps) - 1) < n - 1:
        steps.append(1 << len(steps) - 1)

    def tell(j):
        @pl.when(me >= steps[j])
        def _():
            greet(word.at[2 * j], me - steps[j], probe)

        if j > 0:

            @pl.when(me + steps[j] < n)
            def _():
                greet(word.at[2 * j + 1], me + steps[j], probe)

    def hear(j):
        @pl.when(me + steps[j] < n)
        def _():
            pl.semaphore_wait(word.at[2 * j], 1)

        if j > 0:

            @pl.when(me >= steps[j])
            def _():
                pl.semaphore_wait(word.at[2 * j + 1], 1)

    def hop(src, dst, slot, leaf, row, landing=None):
        return pltpu.make_async_remote_copy(
            src_ref=src, dst_ref=dst, send_sem=hsend.at[slot],
            recv_sem=hrecv.at[slot if landing is None else landing],
            device_id={"leaf": leaf, "probe": row}, device_id_type=MESH,
        )

    pl.semaphore_wait(barrier, 1 + jnp.where(me > 0, 2, 0))
    tell(0)

    point_hop = hop(prow.at[pl.ds(0, REACH)], prow.at[pl.ds(half, REACH)], 0, before, twin)
    rim_hop = hop(leaves(probes_hbm, 0, REACH), into_d(mine, half, REACH), 1, before, even + 1, 1 + mine)
    rim_in = [
        hop(leaves(probes_hbm, 0, REACH), into_d(k, half, REACH), 1, before, even + 1, 1 + k)
        for k in range(2)
    ]
    twin_hop = hop(leaves(probes_hbm, twin_base, half), into_d(mine, 0, half), 3, me, twin)
    ring_hop = hop(leaves(probes_hbm, half, REACH), into_d(mine, half, REACH), 4, me, twin)
    twin_hop.start()

    @pl.when(mine == 1)
    def _():
        ring_hop.start()

    @pl.when(me > 0)
    def _():
        rim_hop.start()

    place = lax.broadcasted_iota(jnp.int32, (width, width), 0)
    for copy in loads[:3]:
        copy.wait()
    c8[...] = jnp.zeros_like(c8)
    c8[0:3, :] = cin[...] * (RATE / TAPER)

    def gather(k):
        x = c8[:, pl.ds(pl.multiple_of((base + k) * width, width), width)]
        parts = three(x, 0)
        onehot = jnp.where(place == order[pl.ds(base + k, 1), :], 1.0, 0.0).astype(BF16)
        got = dot(parts, onehot, 1, 0)
        prow[k] = got[0:8] + got[8:16] + got[16:24]

    for k in range(half):
        gather(k)

    @pl.when(mine == 0)
    def _():
        for k in range(half, span):
            gather(k)

    slots = pairs.shape[1]
    first = pairs[0:1, :]
    second = pairs[1:2, :]
    code = (first - me * leaf_dev - base) * OFFS + (second - first)
    want = lax.broadcasted_iota(jnp.int32, (half * OFFS, slots), 0)
    hit = jnp.max(jnp.where(want == code, RATE, 0.0), axis=1, keepdims=True)
    mask[...] = jnp.broadcast_to(hit, mask.shape)
    acc[...] = jnp.zeros_like(acc)
    acc2[...] = jnp.zeros_like(acc2)

    @pl.when(jnp.logical_and(mine == 0, me > 0))
    def _():
        point_hop.start()

    def both(field, k):
        return jnp.concatenate([field[0, k], field[1, k]], axis=0)

    def probe_rows(r, k):
        return d[r, :, pl.ds(pl.multiple_of(k * width, width), width)]

    def both_probes(k):
        return jnp.concatenate([probe_rows(0, k), probe_rows(1, k)], axis=0)

    def stack(k, x):
        hi = x.astype(BF16)
        v2[k] = jnp.concatenate([hi, (x - hi.astype(F32)).astype(BF16)], axis=0)

    def add(into, k, x):
        into[0, k] += x[:cols]
        into[1, k] += x[cols:]

    rows = 2 * cols

    def tile(s):
        return [
            jnp.concatenate([tiles[s, p, h] for h in range(width // 128)], axis=1)
            for p in range(2)
        ]

    def columns(vi, hi, lo):
        x = dot(vi, hi, 1, 0)
        return x[:rows] + x[rows:] + dot(vi[:rows], lo, 1, 0)

    def products(i, into, make):
        vi = v2[i]
        row = jnp.zeros((2 * rows, width), F32)
        low = jnp.zeros((rows, width), F32)
        for o in [*range(1, OFFS), 0]:
            make(i, o)
            hi, lo = tile(i * OFFS + o)
            vj = v2[i + o]
            if o > 0:
                add(into, i + o, columns(vi, hi, lo))
                row = row + dot(vj, hi, 1, 1)
                low = low + dot(vj[:rows], lo, 1, 1)
            else:
                row = row + dot(vj, hi, 1, 0)
                low = low + dot(vj[:rows], lo, 1, 0)
        add(into, i, row[:rows] + row[rows:] + low)

    def first_products(i):
        vi = v2[i]
        for o in range(OFFS):
            hi, lo = tile(i * OFFS + o)
            x = columns(vi, hi, lo)
            if o > 0:
                add(acc2, i + o, x)
            else:
                diag[i] = x

    def last_products(i):
        row = jnp.zeros((2 * rows, width), F32)
        low = jnp.zeros((rows, width), F32)
        for o in range(1, OFFS):
            hi, lo = tile(i * OFFS + o)
            vj = v2[i + o]
            row = row + dot(vj, hi, 1, 1)
            low = low + dot(vj[:rows], lo, 1, 1)
        add(acc2, i, row[:rows] + row[rows:] + low + diag[i])

    def turn(i):
        turned = prow[i].T
        for c in range(3):
            pcb[c] = jnp.broadcast_to(turned[:, c : c + 1], (width, 128))

    def build(i, o):
        s = i * OFFS + o
        for h in range(width // 128):
            at = slice(h * 128, h * 128 + 128)
            listed = mask[pl.ds(s, 1), :]
            right = [
                jnp.broadcast_to(
                    jnp.where(listed > 0.0, prow[i + o, c : c + 1, at], prow[i, c : c + 1, at]),
                    (ROWS, 128),
                )
                for c in range(3)
            ]
            top = jnp.broadcast_to(listed, (ROWS, 128))
            for a in range(0, width if o > 0 else at.stop, ROWS):
                dx = pcb[0, a : a + ROWS, :] - right[0]
                dy = pcb[1, a : a + ROWS, :] - right[1]
                dz = pcb[2, a : a + ROWS, :] - right[2]
                d2 = jnp.maximum(dx * dx + dy * dy + dz * dz, 1e-30)
                y = jnp.maximum(top - d2 * lax.rsqrt(d2), 0.0)
                y2 = y * y
                t = (y2 * y2) * (y2 + (LIN * y + CON)) * jnp.exp2(y)
                hi = t.astype(BF16)
                tiles[s, 0, h, a : a + ROWS, :] = hi
                tiles[s, 1, h, a : a + ROWS, :] = (t - hi.astype(F32)).astype(BF16)
            if o == 0:
                for p in range(2):
                    for g in range(h):
                        block = tiles[s, p, h, g * 128 : g * 128 + 128, :]
                        tiles[s, p, g, h * 128 : h * 128 + 128, :] = block.T

    for copy in loads[3:]:
        copy.wait()

    @pl.when(mine == 0)
    def _():
        ring_load.wait()

    @pl.when(jnp.logical_and(mine == 1, me == n - 1))
    def _():
        d[:, :, half * width :] = jnp.zeros((2, cols, REACH * width), F32)
        prow[pl.ds(half, REACH)] = jnp.zeros((REACH, 8, width), F32)

    twin_hop.wait_recv()
    for k in range(half):
        stack(k, both_probes(k))

    edge_hops = []
    for j in range(REACH):
        seat = jnp.where(mine == 0, j, REACH - 1 - j)
        edge_hops.append(
            pltpu.make_async_remote_copy(
                src_ref=acc.at[:, edge + seat], dst_ref=in_edge.at[:, seat],
                send_sem=esend.at[seat], recv_sem=erecv.at[seat],
                device_id={"leaf": edge_leaf, "probe": twin}, device_id_type=MESH,
            )
        )
    inner_hop = hop(acc.at[:, pl.ds(inner, REACH)], in_twin, 6, me, twin)
    lag = half - REACH

    def leaf_at(t):
        late = jnp.where(t < AHEAD + REACH, half - 1 + AHEAD - t, t - REACH)
        return jnp.where(mine == 0, t, jnp.where(t < AHEAD, t, late))

    turn(0)

    def first_pass(t, carry):
        i = leaf_at(t)

        @pl.when(t == jnp.where(mine == 0, lag, AHEAD))
        def _():
            @pl.when(mine == 0)
            def _():
                ring_hop.wait_recv()

            @pl.when(jnp.logical_and(mine == 1, me < n - 1))
            def _():
                point_hop.wait_recv()
                for k in range(2):
                    rim_in[k].wait_recv()

            for k in range(half, span):
                stack(k, both_probes(k))

        for j in range(len(steps) - 1):
            @pl.when(t == j + 2)
            def _(j=j):
                hear(j)
                tell(j + 1)

        products(i, acc, build)
        turn(leaf_at(jnp.minimum(t + 1, half - 1)))

        for j in range(REACH):

            @pl.when(jnp.logical_and(t == j + AHEAD * mine, has_edge))
            def _(j=j):
                edge_hops[j].start()

        return carry

    lax.fori_loop(0, half, first_pass, 0)
    inner_hop.start()
    for j in range(half - 2, len(steps) - 1):
        hear(j)
        tell(j + 1)

    @pl.when(jnp.logical_not(has_edge))
    def _():
        in_edge[...] = jnp.zeros_like(in_edge)

    def make_w(k, more):
        xs = []
        for r in range(2):
            x = acc[r, k]
            if more is not None:
                x = x + more[r]
            x = NORM * x - probe_rows(r, k)
            w[r, k] = x
            xs.append(x)
        stack(k, jnp.concatenate(xs, axis=0))

    for k in range(REACH, half):
        make_w(k, None)

    @pl.when(has_edge)
    def _():
        for copy in edge_hops:
            copy.wait_recv()

    for k in range(REACH):
        make_w(edge + k, [in_edge[r, k] for r in range(2)])

    def outer_columns(t, carry):
        first_products(t + REACH * mine)
        return carry

    lax.fori_loop(0, lag, outer_columns, 0, unroll=True)
    inner_hop.wait_recv()
    for k in range(REACH):
        make_w(inner + k, [in_twin[r, k] for r in range(2)])

    far_hop = hop(w.at[other, pl.ds(0, half)], wfar, 7, me, twin)
    far_hop.start()
    give_hop = hop(acc2.at[other, pl.ds(0, half)], part.at[pl.ds(0, half)], 8, me, twin)
    give_rim = hop(acc2.at[other, pl.ds(half, REACH)], part.at[pl.ds(half, REACH)], 9, me, twin)
    next_even = hop(acc2.at[0, pl.ds(half, REACH)], part.at[pl.ds(half, REACH)], 9, after, even)
    next_odd = hop(acc2.at[1, pl.ds(half, REACH)], back, 10, after, even + 1)

    left = lag * other

    hear(len(steps) - 1)
    greet(line_done, me, twin)
    for t in range(REACH):
        first_products(left + REACH - 1 - t)
        if t == 2 * REACH - half - 1:

            @pl.when(jnp.logical_and(mine == 1, me < n - 1))
            def _():
                next_even.start()
                next_odd.start()

    @pl.when(mine == 0)
    def _():
        give_rim.start()


    def lanes(x):
        return x[:, :128] + x[:, 128:] if width == 256 else x

    sums = [jnp.zeros((rows, width), F32) for _ in range(4)]
    own_part = jnp.zeros((rows, width), F32)
    for k in range(span):
        wk = both(w, k)
        sums[3] = sums[3] + wk * both(acc2, k)
        if k < half:
            own_part = own_part + wk * diag[k]
        if k < half:
            dk = both_probes(k)
            sums[0] = sums[0] + dk * dk
            sums[1] = sums[1] + dk * wk
            sums[2] = sums[2] + wk * wk
    sums[3] = 2.0 * sums[3] + own_part
    stacked = jnp.concatenate([lanes(x) for x in sums], axis=0)
    parts = three(stacked, 1)
    total = dot(jnp.full((8, parts.shape[1]), 1.0, BF16), parts, 1, 1)
    sum_out[...] = total[0:1]
    pl.semaphore_wait(line_done, 1)
    copies = []
    for slot, leaf, row in peers:
        copy = pltpu.make_async_remote_copy(
            src_ref=sum_out, dst_ref=sum_in.at[slot],
            send_sem=ssem.at[slot], recv_sem=rsem.at[slot],
            device_id={"leaf": leaf, "probe": row}, device_id_type=MESH,
        )
        copy.start()
        copies.append(copy)

    def last_half(i, carry):
        last_products(i)
        return carry

    lax.fori_loop(0, half, last_half, 0, unroll=4)
    give_hop.start()

    @pl.when(jnp.logical_and(mine == 0, me == 0))
    def _():
        part[pl.ds(half, REACH)] = jnp.zeros((REACH, cols, width), F32)

    @pl.when(jnp.logical_and(mine == 1, me == 0))
    def _():
        back[...] = jnp.zeros_like(back)

    @pl.when(mine == 0)
    def _():
        back[...] = acc2[0, pl.ds(half, REACH)]

    total = sum_out[...]
    for slot, copy in enumerate(copies):
        copy.wait_recv()
        total = total + sum_in[slot]
    column = lax.broadcasted_iota(jnp.int32, (cols, 128), 1)
    line = lax.broadcasted_iota(jnp.int32, (cols, 128), 0) + mine * cols
    rr, dw, ww, wk = [
        jnp.sum(jnp.where(column == line + q * rows, total, 0.0), axis=1, keepdims=True)
        for q in range(4)
    ]
    wz = NORM * wk - ww
    m = dw / rr
    alpha0 = rr / (SHIFT * rr + dw)
    uu = ww - m * dw
    tilt = alpha0 * uu / rr
    alpha1 = uu / (SHIFT * uu + (m * (m * dw - 2.0 * ww) + wz) - tilt * uu)
    e = alpha0 * (m + tilt)
    both_alpha = alpha0 * alpha1
    sol_d = alpha0 + alpha1 * e
    res_d = alpha0 * m - SHIFT * alpha1 * e
    res_w = -(alpha0 + alpha1 * e - SHIFT * both_alpha) - both_alpha
    res_z = both_alpha * NORM

    far_hop.wait_recv()
    give_hop.wait_recv()

    @pl.when(mine == 1)
    def _():
        give_rim.wait_recv()

    @pl.when(jnp.logical_and(mine == 0, me > 0))
    def _():
        next_even.wait_recv()

    @pl.when(jnp.logical_and(mine == 1, me > 0))
    def _():
        next_odd.wait_recv()

    def finish(l, dl, wl, zl):
        at = pl.ds(pl.multiple_of(l * width, width), width)
        out_ref[0, :, at] = sol_d * dl
        out_ref[1, :, at] = both_alpha * wl
        out_ref[2, :, at] = res_d * dl + res_w * wl
        out_ref[3, :, at] = res_z * zl

    for k in range(half):
        near = acc2[mine, k]
        far = part[k]
        if k < REACH:
            near = near + part[half + k]
            far = far + back[k]
        finish(base + k, probe_rows(mine, k), w[mine, k], near)
        finish(twin_base + k, own[:, k * width : (k + 1) * width], wfar[k], far)

    for copy in copies:
        copy.wait_send()
    for copy in (twin_hop, inner_hop, far_hop, give_hop):
        copy.wait_send()

    @pl.when(mine == 1)
    def _():
        ring_hop.wait_send()

    @pl.when(mine == 0)
    def _():
        give_rim.wait_send()

    @pl.when(jnp.logical_and(mine == 0, me > 0))
    def _():
        point_hop.wait_send()

    @pl.when(me > 0)
    def _():
        rim_hop.wait_send()

    @pl.when(has_edge)
    def _():
        for copy in edge_hops:
            copy.wait_send()

    @pl.when(jnp.logical_and(mine == 1, me < n - 1))
    def _():
        next_even.wait_send()
        next_odd.wait_send()


def body(coords, site_order, leaf_pairs, pair_count, probes):
    arrays = (coords, site_order, leaf_pairs, probes)
    n = lax.axis_size("leaf")
    leaf_dev, width = site_order.shape
    cols = probes.shape[0]
    half = leaf_dev // 2
    span = half + REACH
    slots_in = 2 * n - 1
    hbm = pl.BlockSpec(memory_space=pltpu.HBM)
    vmem = pl.BlockSpec(memory_space=pltpu.VMEM)
    field = functools.partial(pltpu.VMEM, dtype=F32)
    terms = pl.pallas_call(
        functools.partial(kernel, n),
        out_shape=jax.ShapeDtypeStruct((4, *probes.shape), F32),
        in_specs=[hbm] * 4,
        out_specs=vmem,
        scratch_shapes=[
            field(coords.shape),
            pltpu.VMEM(site_order.shape, jnp.int32),
            pltpu.VMEM(leaf_pairs.shape, jnp.int32),
            field((cols, half * width)),
            field((8, leaf_dev * width)),
            field((span, 8, width)),
            field((3, width, 128)),
            field((half * OFFS, 128)),
            pltpu.VMEM((half * OFFS, 2, width // 128, width, 128), BF16),
            field((2, cols, span * width)),
            field((2, span, cols, width)),
            field((half, cols, width)),
            pltpu.VMEM((span, 4 * cols, width), BF16),
            field((2, span, cols, width)),
            field((2, span, cols, width)),
            field((2, REACH, cols, width)),
            field((2, REACH, cols, width)),
            field((span, cols, width)),
            field((REACH, cols, width)),
            field((half, 2 * cols, width)),
            field((1, 128)),
            field((slots_in, 1, 128)),
            pltpu.SemaphoreType.REGULAR((2 * n.bit_length() + 2,)),
            pltpu.SemaphoreType.REGULAR,
            pltpu.SemaphoreType.DMA((6,)),
            pltpu.SemaphoreType.DMA((slots_in,)),
            pltpu.SemaphoreType.DMA((slots_in,)),
            pltpu.SemaphoreType.DMA((11,)),
            pltpu.SemaphoreType.DMA((11,)),
            pltpu.SemaphoreType.DMA((REACH,)),
            pltpu.SemaphoreType.DMA((REACH,)),
        ],
        compiler_params=pltpu.CompilerParams(
            collective_id=0, has_side_effects=True, vmem_limit_bytes=48 * 2**20
        ),
    )(*[pltpu.with_memory_space_constraint(x, pltpu.HBM) for x in arrays])

    return terms[0] - terms[1], terms[2] + terms[3]


def solution(mesh):
    in_specs = (P(None, "leaf"), P("leaf", None), P(None, "leaf"), P("leaf"), P("probe", "leaf"))
    out_specs = (P("probe", "leaf"), P("probe", "leaf"))
    return jax.shard_map(body, mesh=mesh, in_specs=in_specs, out_specs=out_specs, check_vma=False)
```
